128 devices in a mesh: graph: 32 (over z, x, core), batch: 4 (over y).
Axes of the slice: x: 4, y: 4, z: 4, core: 2. Of those that a mesh axis runs over, the one named last changes fastest.
Arguments:
- node_latent: bfloat16 [4, 4096, 512], P('batch', 'graph'), may hold values from -6 to 6
- edge_latent: bfloat16 [4, 32768, 512], P('batch', 'graph'), may hold values from -6 to 6
- node_cotangent: bfloat16 [4, 4096, 512], P('batch', 'graph'), may hold values from -6 to 6
- edge_w_in: bfloat16 [2, 1536, 512], replicated, may hold values from -0.15625 to 0.15625
- edge_w_out: bfloat16 [2, 512, 512], replicated, may hold values from -0.25 to 0.25
- node_w_in: bfloat16 [2, 1024, 512], replicated, may hold values from -0.1875 to 0.1875
- node_w_out: bfloat16 [2, 512, 512], replicated, may hold values from -0.25 to 0.25
- edge_gain: float32 [2, 512], replicated, may hold values from 0.25 to 1.75
- node_gain: float32 [2, 512], replicated, may hold values from 0.25 to 1.75
- edge_slot: int32 [32768], P('graph'), may hold values from 0 to 1151, as said below
- edge_receiver: int32 [32768], P('graph'), may hold values from 0 to 127
- send_list: int32 [1024, 32], P('graph'), may hold values from 0 to 127, as said below
- edge_count: int32 [32], P('graph'), may hold values from 256 to 1024, as said below
Outputs:
- node_out: float32 [4, 4096, 512], P('batch', 'graph')
- node_grad: float32 [4, 4096, 512], P('batch', 'graph')
- grad_edge_in: float32 [2, 1536, 512], P(None, ('graph', 'batch'))
- grad_edge_out: float32 [2, 512, 512], P(None, ('graph', 'batch'))
- grad_node_in: float32 [2, 1024, 512], P(None, ('graph', 'batch'))
- grad_node_out: float32 [2, 512, 512], P(None, ('graph', 'batch'))
- grad_edge_gain: float32 [2, 512], P(None, ('graph', 'batch'))
- grad_node_gain: float32 [2, 512], P(None, ('graph', 'batch'))
The draws below stay inside these ranges and needn't reach their ends.
Inputs may be any that keep to these rules, and one draw needn't show every extreme that they name: `edge_slot`: for edge j of partition p = j // 1024: a slot below 128 names a node of partition p; a slot s of 128 or more names row (s - 128) % 32 of the list that partition q = (s - 128) // 32 keeps for partition p, and q differs from p cyclically by 1 to 2 steps or by exactly 32 // 2 steps. `edge_receiver`: the receiving node is a node of the edge's own partition. `send_list`: row q * 32 + p holds 32 distinct node numbers within partition q, the nodes whose latents partition p may read. `edge_count`: edge slots at or above a partition's count carry no edge.
All inputs are finite; a program needn't handle non-finite values.
Results may differ from the reference program's by a relative error of at most 0.035.
Values may be sent and summed in bfloat16 or wider, within the bound.
No kernel may reach another device: no remote copies, remote signals or barrier semaphores. Data moves between devices by JAX's collectives and lax.ppermute only.
A program may use at most 128 MiB of HBM per device.

```python
import jax
import jax.numpy as jnp
from jax import lax

D = 512
HID = 512
LAYERS = 2
HOPS = 2
NOD_DEV = 128
EDGE_CAP = 1024
PEER_CAP = 32
NODES = 4096
EDGES = 32768
SAMPLES = 4
N_GRAPH = 32


def draw_edge_slot(key, part):
    subkeys = jax.random.split(jax.random.fold_in(key, 11), 4)
    edge_ids = jnp.arange(EDGES, dtype=jnp.int32)
    owner = edge_ids // EDGE_CAP
    is_local = jax.random.randint(subkeys[0], (EDGES,), 0, 2) == 0
    local_slot = jax.random.randint(subkeys[1], (EDGES,), 0, NOD_DEV)
    hop_pick = jax.random.randint(subkeys[2], (EDGES,), 0, 2 * HOPS + 1)
    offset = jnp.where(hop_pick < HOPS, hop_pick - HOPS, jnp.where(hop_pick < 2 * HOPS, hop_pick - HOPS + 1, N_GRAPH // 2))
    source = (owner + offset) % N_GRAPH
    within = jax.random.randint(subkeys[3], (EDGES,), 0, PEER_CAP)
    return jnp.where(is_local, local_slot, NOD_DEV + source * PEER_CAP + within).astype(jnp.int32)


def draw_send_list(key, part):
    subkeys = jax.random.split(jax.random.fold_in(key, 23), N_GRAPH * N_GRAPH)

    def one_list(row_key):
        return jax.random.permutation(row_key, NOD_DEV)[:PEER_CAP]
    return jax.vmap(one_list)(subkeys).astype(jnp.int32)


def draw_edge_count(key, part):
    subkeys = jax.random.split(jax.random.fold_in(key, 37), 2)
    counts = jax.random.randint(subkeys[0], (N_GRAPH,), EDGE_CAP // 4, EDGE_CAP + 1)
    fullest = jax.random.randint(subkeys[1], (), 0, N_GRAPH)
    return jnp.where(jnp.arange(N_GRAPH) == fullest, EDGE_CAP, counts).astype(jnp.int32)


def with_ends(array, stream_key, smallest, top_value):
    shape = array.shape
    index_at = [jax.random.randint(jax.random.fold_in(stream_key, axis), (), 0, shape[axis]) for axis in range(len(shape))]
    array = array.at[tuple(index_at)].set(smallest)
    longest = shape.index(max(shape))
    index_at[longest] = (index_at[longest] + 1) % shape[longest]
    return array.at[tuple(index_at)].set(top_value)


def shard_levels(stream_key, shape, cuts, low, largest):
    level = 1.0
    for position, blocks in cuts:
        heights = jax.random.uniform(jax.random.fold_in(jax.random.fold_in(stream_key, 6), position), (blocks,), jnp.float32, low / len(cuts), largest / len(cuts))
        level = level * jnp.repeat(jnp.exp(heights), shape[position] // blocks).reshape((-1,) + (1,) * (len(shape) - 1 - position))
    return level


def noise(own_key, shape, spread, most, cuts=(), held_as=jnp.bfloat16):
    array = spread * jax.random.normal(own_key, shape, jnp.float32)
    if cuts:
        array = array * shard_levels(own_key, shape, cuts, -0.22, 0.18)
    return jnp.clip(array, -most, most).astype(held_as)


def setup_inputs(seed: int = 0) -> dict:
    keys = jax.random.split(jax.random.key(seed), 14)
    node_latent = noise(keys[0], (SAMPLES, NODES, D), 1.0, 6.0, ((0, 4), (1, 32)))
    edge_latent = noise(keys[1], (SAMPLES, EDGES, D), 1.0, 6.0, ((0, 4), (1, 32)))
    node_cotangent = noise(keys[2], (SAMPLES, NODES, D), 1.0, 6.0, ((0, 4), (1, 32)))
    edge_w_in = noise(keys[3], (LAYERS, 3 * D, HID), (3 * D) ** -0.5, 0.15625)
    edge_w_out = noise(keys[4], (LAYERS, HID, D), HID ** -0.5, 0.25)
    node_w_in = noise(keys[5], (LAYERS, 2 * D, HID), (2 * D) ** -0.5, 0.1875)
    node_w_out = noise(keys[6], (LAYERS, HID, D), HID ** -0.5, 0.25)
    edge_gain = jnp.clip(1.0 + 0.15 * jax.random.normal(keys[7], (LAYERS, D), jnp.float32), 0.25, 1.75)
    node_gain = jnp.clip(1.0 + 0.15 * jax.random.normal(keys[8], (LAYERS, D), jnp.float32), 0.25, 1.75)
    edge_slot = draw_edge_slot(jax.random.fold_in(keys[13], 71), 0)
    edge_receiver = with_ends(jax.random.randint(keys[10], (EDGES,), 0, NOD_DEV), jax.random.fold_in(keys[10], 1), 0, NOD_DEV - 1).astype(jnp.int32)
    send_list = draw_send_list(jax.random.fold_in(keys[13], 71), 0)
    edge_count = draw_edge_count(jax.random.fold_in(keys[13], 71), 0)
    return {"node_latent": node_latent, "edge_latent": edge_latent, "node_cotangent": node_cotangent, "edge_w_in": edge_w_in, "edge_w_out": edge_w_out, "node_w_in": node_w_in, "node_w_out": node_w_out, "edge_gain": edge_gain, "node_gain": node_gain, "edge_slot": edge_slot, "edge_receiver": edge_receiver, "send_list": send_list, "edge_count": edge_count}


EPSILON = 1e-05

def mlp_forward(pieces, weights, w_out, gain, live):
    pre_act = None
    for piece, weight in zip(pieces, weights):
        term = jnp.dot(piece, weight, preferred_element_type=jnp.float32)
        pre_act = term if pre_act is None else pre_act + term
    hidden = (pre_act * jax.nn.sigmoid(pre_act)).astype(jnp.bfloat16)
    projected = jnp.dot(hidden, w_out, preferred_element_type=jnp.float32)
    centre = projected - lax.optimization_barrier(jnp.mean(projected, axis=-1, keepdims=True))
    inv_std = lax.rsqrt(lax.optimization_barrier(jnp.mean(centre * centre, axis=-1, keepdims=True)) + EPSILON)
    normed = centre * inv_std
    result = normed * gain
    if live is not None:
        result = result * live[:, None]
    return (result, (pre_act, hidden, normed, inv_std))

def mlp_backward(grad_out, pieces, weights, w_out, gain, live, saved):
    pre_act, hidden, normed, inv_std = saved
    if live is not None:
        grad_out = grad_out * live[:, None]
    grad_gain = lax.optimization_barrier(jnp.sum(grad_out * normed, axis=0))
    grad_norm = grad_out * gain
    grad_proj = inv_std * (grad_norm - lax.optimization_barrier(jnp.mean(grad_norm, axis=-1, keepdims=True)) - normed * lax.optimization_barrier(jnp.mean(grad_norm * normed, axis=-1, keepdims=True)))
    grad_proj_bf = grad_proj.astype(jnp.bfloat16)
    grad_w_out = jnp.dot(hidden.T, grad_proj_bf, preferred_element_type=jnp.float32)
    grad_hidden = jnp.dot(grad_proj_bf, w_out.T, preferred_element_type=jnp.float32)
    sigma = jax.nn.sigmoid(pre_act)
    grad_pre = grad_hidden * sigma * (1.0 + pre_act * (1.0 - sigma))
    grad_pre_bf = grad_pre.astype(jnp.bfloat16)
    grad_weights = [jnp.dot(piece.T, grad_pre_bf, preferred_element_type=jnp.float32) for piece in pieces]
    grad_pieces = [jnp.dot(grad_pre_bf, weight.T, preferred_element_type=jnp.float32) for weight in weights]
    return (grad_pieces, grad_weights, grad_w_out, grad_gain)

def run_sample(node_start, edge_start, cotangent, edge_w_in, edge_w_out, node_w_in, node_w_out, edge_gain, node_gain, sender, receiver, live):
    state = node_start.astype(jnp.float32)
    edge_state = edge_start.astype(jnp.float32)
    edge_bf = edge_start
    records = []
    for layer in range(LAYERS):
        node_bf = state.astype(jnp.bfloat16)
        if layer > 0:
            edge_bf = edge_state.astype(jnp.bfloat16)
        from_sender = node_bf[sender]
        at_receiver = node_bf[receiver]
        w_first = edge_w_in[layer]
        edge_weights = [w_first[:D], w_first[2 * D:], w_first[D:2 * D]]
        edge_inputs = [edge_bf, at_receiver, from_sender]
        message, edge_saved = mlp_forward(edge_inputs, edge_weights, edge_w_out[layer], edge_gain[layer], live)
        summed = jax.ops.segment_sum(message, receiver, num_segments=NODES).astype(jnp.bfloat16)
        n_first = node_w_in[layer]
        node_weights = [n_first[:D], n_first[D:]]
        node_inputs = [node_bf, summed]
        update, node_saved = mlp_forward(node_inputs, node_weights, node_w_out[layer], node_gain[layer], None)
        records.append((edge_inputs, edge_weights, edge_saved, node_inputs, node_weights, node_saved))
        edge_state = edge_state + message
        state = state + update
    grad_state = cotangent.astype(jnp.float32)
    grad_edge = None
    layer_grads = []
    for layer in reversed(range(LAYERS)):
        edge_inputs, edge_weights, edge_saved, node_inputs, node_weights, node_saved = records[layer]
        node_parts, node_wgrads, grad_n_out, grad_n_gain = mlp_backward(grad_state, node_inputs, node_weights, node_w_out[layer], node_gain[layer], None, node_saved)
        grad_message = node_parts[1][receiver]
        if grad_edge is not None:
            grad_message = grad_message + grad_edge
        edge_parts, edge_wgrads, grad_e_out, grad_e_gain = mlp_backward(grad_message, edge_inputs, edge_weights, edge_w_out[layer], edge_gain[layer], live, edge_saved)
        grad_edge = edge_parts[0] if grad_edge is None else edge_parts[0] + grad_edge
        grad_state = grad_state + node_parts[0] + jax.ops.segment_sum(edge_parts[1], receiver, num_segments=NODES) + jax.ops.segment_sum(edge_parts[2], sender, num_segments=NODES)
        grad_e_in = jnp.concatenate([edge_wgrads[0], edge_wgrads[2], edge_wgrads[1]], axis=0)
        grad_n_in = jnp.concatenate([node_wgrads[0], node_wgrads[1]], axis=0)
        layer_grads.append((grad_e_in, grad_e_out, grad_n_in, grad_n_out, grad_e_gain, grad_n_gain))
    layer_grads = layer_grads[::-1]
    stacked = tuple((jnp.stack([entry[index] for entry in layer_grads]) for index in range(6)))
    return (state, grad_state) + stacked

def reference(node_latent, edge_latent, node_cotangent, edge_w_in, edge_w_out, node_w_in, node_w_out, edge_gain, node_gain, edge_slot, edge_receiver, send_list, edge_count):
    edge_ids = jnp.arange(EDGES, dtype=jnp.int32)
    owner = edge_ids // EDGE_CAP
    is_local = edge_slot < NOD_DEV
    remote = jnp.where(is_local, 0, edge_slot - NOD_DEV).astype(jnp.int32)
    source = remote // PEER_CAP
    within = remote % PEER_CAP
    listed = send_list[source * N_GRAPH + owner, within]
    sender = jnp.where(is_local, owner * NOD_DEV + edge_slot, source * NOD_DEV + listed).astype(jnp.int32)
    receiver = (owner * NOD_DEV + edge_receiver).astype(jnp.int32)
    live = (edge_ids % EDGE_CAP < edge_count[owner]).astype(jnp.float32)

    def sample_fn(inputs):
        node_start, edge_start, cotangent = inputs
        return run_sample(node_start, edge_start, cotangent, edge_w_in, edge_w_out, node_w_in, node_w_out, edge_gain, node_gain, sender, receiver, live)
    results = lax.map(sample_fn, (node_latent, edge_latent, node_cotangent))
    node_out, node_grad = (results[0], results[1])
    sums = tuple((lax.optimization_barrier(jnp.sum(entry, axis=0)) for entry in results[2:]))
    return (node_out, node_grad, sums[0], sums[1], sums[2], sums[3], sums[4], sums[5])
```

```python
import functools

import jax
import jax.numpy as jnp
from jax import lax
from jax.experimental import pallas as pl
from jax.experimental.pallas import tpu as pltpu
from jax.sharding import PartitionSpec as P

HOPS = 2
EPSILON = 1e-05
CHUNK = 256
OFFSETS = (-2, -1, 1, 2, 16)
F32 = jnp.float32
BF16 = jnp.bfloat16


def nn(a, b):
    return lax.dot_general(a, b, (((1,), (0,)), ((), ())), preferred_element_type=F32)


def nt(a, b):
    return lax.dot_general(a, b, (((1,), (1,)), ((), ())), preferred_element_type=F32)


def tn(a, b):
    return lax.dot_general(a, b, (((0,), (0,)), ((), ())), preferred_element_type=F32)


def sigmoid(x):
    return 0.5 * jnp.tanh(0.5 * x) + 0.5


def layer_norm(z):
    centre = z - jnp.mean(z, axis=-1, keepdims=True)
    inv = lax.rsqrt(jnp.mean(centre * centre, axis=-1, keepdims=True) + EPSILON)
    return centre * inv, inv


def layer_norm_back(grad, gain, normed, inv):
    gn = grad * gain
    m1 = jnp.mean(gn, axis=-1, keepdims=True)
    m2 = jnp.mean(gn * normed, axis=-1, keepdims=True)
    return inv * (gn - m1 - normed * m2)


def swish_back(pre):
    s = sigmoid(pre)
    return s * (1.0 + pre * (1.0 - s))


def list_onehot(lists_ref, own, offset, nodes):
    row = lists_ref[pl.ds((own - offset) & 31, 1), :]
    ids = lax.broadcasted_iota(jnp.int32, (nodes, row.shape[1]), 0)
    return jnp.where(ids == row, 1.0, 0.0).astype(BF16)


def send_blocks(lists_ref, own, vb, outs):
    for offset, out in zip(OFFSETS, outs):
        onehot = list_onehot(lists_ref, own, offset, vb.shape[0])
        out[...] = tn(onehot, vb).astype(BF16)


def returned(lists_ref, own, blocks):
    total = None
    for offset, block in zip(OFFSETS, blocks):
        term = nn(list_onehot(lists_ref, own, offset, 128), block[...])
        total = term if total is None else total + term
    return total


def build_onehot(onehot_ref, slot_ref, receiver_ref, own):
    edges = slot_ref.shape[1]
    slot = slot_ref[...]
    row = slot - 128
    distance = ((row >> 5) - own) & 31
    block = jnp.where(distance == 30, 0, jnp.where(distance == 31, 1, jnp.where(distance == 1, 2, jnp.where(distance == 2, 3, 4))))
    position = jnp.where(slot < 128, slot, 128 + block * 32 + (row & 31))
    ids = lax.broadcasted_iota(jnp.int32, (128, edges), 0)
    onehot_ref[0:128, :] = jnp.where(ids == receiver_ref[...], 1.0, 0.0).astype(BF16)
    ids = lax.broadcasted_iota(jnp.int32, (384, edges), 0)
    onehot_ref[128:512, :] = jnp.where(ids == position, 1.0, 0.0).astype(BF16)


def fill_senders(sender_ref, vb, blocks):
    sender_ref[0:128, :] = vb
    for n, block in enumerate(blocks):
        sender_ref[128 + 32 * n : 160 + 32 * n, :] = block[...]


def fill_projected(layer, proj_ref, vb, sender_ref, w_in_ref):
    proj_ref[0:128, :] = nn(vb, w_in_ref[layer, 1024:1536, :]).astype(BF16)
    proj_ref[128:416, :] = nn(sender_ref[...], w_in_ref[layer, 512:1024, :]).astype(BF16)
    proj_ref[416:512, :] = jnp.zeros((96, 512), BF16)


def live_rows(base, count):
    rows = base + lax.broadcasted_iota(jnp.int32, (CHUNK, 1), 0)
    return jnp.where(rows < count, 1.0, 0.0).astype(F32)


def node_forward(layer, vb, agg, w_in_ref, w_out_ref):
    pre = nn(vb, w_in_ref[layer, 0:512, :]) + nn(agg, w_in_ref[layer, 512:1024, :])
    hidden = (pre * sigmoid(pre)).astype(BF16)
    normed, inv = layer_norm(nn(hidden, w_out_ref[layer]))
    return pre, hidden, normed, inv


def split_store(k, scratch_ref, keep_ref, send_ref, at, rows):
    for c in range(16):
        mine = pl.multiple_of(2 * c * rows + k * rows, 16)
        other = pl.multiple_of(2 * c * rows + (1 - k) * rows, 16)
        keep_ref[c, at : at + rows, :] = scratch_ref[pl.ds(mine, rows), :]
        send_ref[c, at : at + rows, :] = scratch_ref[pl.ds(other, rows), :]


def store_gains(edge_gain, node_gain, keep_ref, send_ref):
    pad = jnp.concatenate([edge_gain, node_gain, jnp.zeros((14, 512), F32)], axis=0).astype(BF16)
    keep_ref[16, 0:16, :] = pad
    send_ref[16, 0:16, :] = pad


def node_backward(layer, grad, vb, agg, pre, hidden, normed, inv, w_in_ref, w_out_ref, gain, g_in_ref, g_out_ref):
    grad_gain = jnp.sum(grad * normed, axis=0, keepdims=True)
    dz = layer_norm_back(grad, gain, normed, inv).astype(BF16)
    g_out_ref[...] = tn(hidden, dz).astype(BF16)
    da = (nt(dz, w_out_ref[layer]) * swish_back(pre)).astype(BF16)
    g_in_ref[0:512, :] = tn(vb, da).astype(BF16)
    g_in_ref[512:1024, :] = tn(agg, da).astype(BF16)
    return grad_gain, nt(da, w_in_ref[layer, 0:512, :]), nt(da, w_in_ref[layer, 512:1024, :])


def gather_kernel(own_ref, lists_ref, vb_ref, *outs):
    send_blocks(lists_ref, own_ref[0], vb_ref[0], outs)


def forward_kernel(
    own_ref, count_ref, lists_ref, slot_ref, receiver_ref, vb_ref, eb_ref, b0, b1, b2, b3, b4,
    we_in, we_out, wn_in, wn_out, e_gain_ref, n_gain_ref,
    v_out, vb_out, eb_out, pre_out, normed_out, inv_out, n_pre_out, n_normed_out, n_inv_out, agg_out,
    o0, o1, o2, o3, o4,
    onehot, senders, proj, message,
):
    own, count = own_ref[0], count_ref[0]
    build_onehot(onehot, slot_ref, receiver_ref, own)
    vb = vb_ref[0]
    fill_senders(senders, vb, (b0, b1, b2, b3, b4))
    fill_projected(0, proj, vb, senders, we_in)
    gain = e_gain_ref[0:1, :]
    for n in range(eb_ref.shape[1] // CHUNK):
        rows = slice(n * CHUNK, (n + 1) * CHUNK)
        eb = eb_ref[0, rows, :]
        pre = nn(eb, we_in[0, 0:512, :]) + tn(onehot[:, rows], proj[...])
        hidden = (pre * sigmoid(pre)).astype(BF16)
        normed, inv = layer_norm(nn(hidden, we_out[0]))
        m = normed * gain * live_rows(n * CHUNK, count)
        pre_out[rows, :] = pre.astype(BF16)
        normed_out[rows, :] = normed.astype(BF16)
        inv_out[rows, :] = jnp.broadcast_to(inv, (CHUNK, 128))
        message[rows, :] = m.astype(BF16)
        eb_out[rows, :] = (eb.astype(F32) + m).astype(BF16)
    agg = nn(onehot[0:128, :], message[...]).astype(BF16)
    pre, _, normed, inv = node_forward(0, vb, agg, wn_in, wn_out)
    v = vb.astype(F32) + normed * n_gain_ref[0:1, :]
    v_out[...] = v
    vb1 = v.astype(BF16)
    vb_out[...] = vb1
    n_pre_out[...] = pre
    n_normed_out[...] = normed
    n_inv_out[...] = jnp.broadcast_to(inv, (128, 128))
    agg_out[...] = agg
    send_blocks(lists_ref, own, vb1, (o0, o1, o2, o3, o4))


def edge_tail(layer, onehot, senders, vb, eb, h_ref, dz_ref, da_ref, we_in, g_in, g_out, outs):
    g_out[...] = tn(h_ref[...], dz_ref[...]).astype(BF16)
    g_in[0:512, :] = tn(eb, da_ref[...]).astype(BF16)
    gathered = nn(onehot[0:416, :], da_ref[...]).astype(BF16)
    at_receiver = gathered[0:128, :]
    at_sender = gathered[128:416, :]
    g_in[512:1024, :] = tn(senders[...], at_sender).astype(BF16)
    g_in[1024:1536, :] = tn(vb, at_receiver).astype(BF16)
    back = nt(at_sender, we_in[layer, 512:1024, :])
    for n, out in enumerate(outs):
        out[...] = back[128 + 32 * n : 160 + 32 * n, :].astype(BF16)
    return nt(at_receiver, we_in[layer, 1024:1536, :]) + back[0:128, :]


def write_grads(k, g_in, g_out, gn_in, gn_out, edge_gain, node_gain, keep, send):
    split_store(k, g_in, keep, send, 0, 48)
    split_store(k, g_out, keep, send, 48, 16)
    split_store(k, gn_in, keep, send, 64, 32)
    split_store(k, gn_out, keep, send, 96, 16)
    store_gains(edge_gain, node_gain, keep, send)


def middle_kernel(
    own_ref, count_ref, slot_ref, receiver_ref, v_ref, vb_ref, eb_ref, cot_ref, b0, b1, b2, b3, b4,
    we_in, we_out, wn_in, wn_out, e_gain_ref, n_gain_ref,
    node_out, grad_out, edge_grad_out, keep, send, o0, o1, o2, o3, o4,
    onehot, senders, proj, message, pre_s, normed_s, inv_s, hidden_s, dz_s, da_s, g_in, g_out, gn_in, gn_out,
):
    own, count = own_ref[0], count_ref[0]
    build_onehot(onehot, slot_ref, receiver_ref, own)
    vb = vb_ref[...]
    fill_senders(senders, vb, (b0, b1, b2, b3, b4))
    fill_projected(1, proj, vb, senders, we_in)
    gain = e_gain_ref[1:2, :]
    chunks = eb_ref.shape[0] // CHUNK
    for n in range(chunks):
        rows = slice(n * CHUNK, (n + 1) * CHUNK)
        pre = nn(eb_ref[rows, :], we_in[1, 0:512, :]) + tn(onehot[:, rows], proj[...])
        hidden = (pre * sigmoid(pre)).astype(BF16)
        normed, inv = layer_norm(nn(hidden, we_out[1]))
        m = normed * gain * live_rows(n * CHUNK, count)
        pre_s[rows, :] = pre
        normed_s[rows, :] = normed
        inv_s[rows, :] = jnp.broadcast_to(inv, (CHUNK, 128))
        hidden_s[rows, :] = hidden
        message[rows, :] = m.astype(BF16)
    agg = nn(onehot[0:128, :], message[...]).astype(BF16)
    n_pre, n_hidden, n_normed, n_inv = node_forward(1, vb, agg, wn_in, wn_out)
    n_gain = n_gain_ref[1:2, :]
    node_out[0] = v_ref[...] + n_normed * n_gain
    grad = cot_ref[0].astype(F32)
    grad_n_gain, grad_v, grad_agg = node_backward(
        1, grad, vb, agg, n_pre, n_hidden, n_normed, n_inv, wn_in, wn_out, n_gain, gn_in, gn_out
    )
    grad_agg = grad_agg.astype(BF16)
    grad_e_gain = jnp.zeros((1, 512), F32)
    for n in range(chunks):
        rows = slice(n * CHUNK, (n + 1) * CHUNK)
        gm = tn(onehot[0:128, rows], grad_agg) * live_rows(n * CHUNK, count)
        normed = normed_s[rows, :]
        grad_e_gain += jnp.sum(gm * normed, axis=0, keepdims=True)
        dz = layer_norm_back(gm, gain, normed, inv_s[rows, 0:1]).astype(BF16)
        dz_s[rows, :] = dz
        da = (nt(dz, we_out[1]) * swish_back(pre_s[rows, :])).astype(BF16)
        da_s[rows, :] = da
        edge_grad_out[rows, :] = nt(da, we_in[1, 0:512, :]).astype(BF16)
    grad_ends = edge_tail(1, onehot, senders, vb, eb_ref[...], hidden_s, dz_s, da_s, we_in, g_in, g_out, (o0, o1, o2, o3, o4))
    grad_out[...] = grad + grad_v + grad_ends
    write_grads(own & 1, g_in, g_out, gn_in, gn_out, grad_e_gain, grad_n_gain, keep, send)


def backward_kernel(
    own_ref, count_ref, lists_ref, slot_ref, receiver_ref, vb_ref, eb_ref, s0, s1, s2, s3, s4,
    grad_ref, r0, r1, r2, r3, r4, edge_grad_ref, pre_ref, normed_ref, inv_ref, n_pre_ref, n_normed_ref, n_inv_ref, agg_ref,
    we_in, we_out, wn_in, wn_out, e_gain_ref, n_gain_ref,
    grad_out, keep, send, o0, o1, o2, o3, o4,
    onehot, senders, hidden_s, dz_s, da_s, g_in, g_out, gn_in, gn_out,
):
    own, count = own_ref[0], count_ref[0]
    build_onehot(onehot, slot_ref, receiver_ref, own)
    vb = vb_ref[0]
    fill_senders(senders, vb, (s0, s1, s2, s3, s4))
    grad = grad_ref[...] + returned(lists_ref, own, (r0, r1, r2, r3, r4))
    n_pre = n_pre_ref[...]
    n_hidden = (n_pre * sigmoid(n_pre)).astype(BF16)
    grad_n_gain, grad_v, grad_agg = node_backward(
        0, grad, vb, agg_ref[...], n_pre, n_hidden, n_normed_ref[...], n_inv_ref[:, 0:1], wn_in, wn_out, n_gain_ref[0:1, :], gn_in, gn_out
    )
    grad_agg = grad_agg.astype(BF16)
    gain = e_gain_ref[0:1, :]
    grad_e_gain = jnp.zeros((1, 512), F32)
    for n in range(eb_ref.shape[1] // CHUNK):
        rows = slice(n * CHUNK, (n + 1) * CHUNK)
        gm = tn(onehot[0:128, rows], grad_agg) + edge_grad_ref[rows, :].astype(F32)
        gm = gm * live_rows(n * CHUNK, count)
        normed = normed_ref[rows, :].astype(F32)
        grad_e_gain += jnp.sum(gm * normed, axis=0, keepdims=True)
        dz = layer_norm_back(gm, gain, normed, inv_ref[rows, 0:1]).astype(BF16)
        dz_s[rows, :] = dz
        pre = pre_ref[rows, :].astype(F32)
        s = sigmoid(pre)
        hidden_s[rows, :] = (pre * s).astype(BF16)
        da_s[rows, :] = (nt(dz, we_out[0]) * (s * (1.0 + pre * (1.0 - s)))).astype(BF16)
    grad_ends = edge_tail(0, onehot, senders, vb, eb_ref[0], hidden_s, dz_s, da_s, we_in, g_in, g_out, (o0, o1, o2, o3, o4))
    grad_out[...] = grad + grad_v + grad_ends
    write_grads(own & 1, g_in, g_out, gn_in, gn_out, grad_e_gain, grad_n_gain, keep, send)


def pack_kernel(keep_ref, recv_ref, out_ref, stage):
    gains = (keep_ref[16, 0:16, :].astype(F32) + recv_ref[16, 0:16, :].astype(F32))[0:8, :]

    def step(c, carry):
        rows = keep_ref[c].astype(F32) + recv_ref[c].astype(F32)
        for b in range(4):
            stage[b, 0:12, :] = rows[12 * b : 12 * b + 12, :]
            stage[b, 12:16, :] = rows[48 + 4 * b : 52 + 4 * b, :]
            stage[b, 16:24, :] = rows[64 + 8 * b : 72 + 8 * b, :]
            stage[b, 24:28, :] = rows[96 + 4 * b : 100 + 4 * b, :]
            stage[b, 28:32, :] = gains[0:4, :]
            out_ref[4 * c + b] = stage[b].astype(BF16)
        return carry

    lax.fori_loop(0, 16, step, 0)


def finish_kernel(
    device_ref, own_ref, lists_ref, grad_ref, r0, r1, r2, r3, r4, x0_ref, x1_ref,
    node_grad, g_e_in, g_e_out, g_n_in, g_n_out, g_e_gain, g_n_gain,
    stage,
):
    node_grad[0] = grad_ref[...] + returned(lists_ref, own_ref[0], (r0, r1, r2, r3, r4))
    picks = lax.broadcasted_iota(jnp.int32, (512, 128), 0) - 4 * device_ref[0]
    select = jnp.where(picks == lax.broadcasted_iota(jnp.int32, (512, 128), 1), 1.0, 0.0).astype(F32)
    for layer, x_ref in enumerate((x0_ref, x1_ref)):

        def step(n, total, x_ref=x_ref):
            return total + x_ref[n].astype(F32)

        stage[...] = lax.fori_loop(0, 64, step, jnp.zeros((32, 512), F32), unroll=8)
        g_e_in[layer] = stage[0:12, :]
        g_e_out[layer] = stage[12:16, :]
        g_n_in[layer] = stage[16:24, :]
        g_n_out[layer] = stage[24:28, :]
        gains = lax.dot_general(
            stage[24:32, :], select, (((1,), (0,)), ((), ())), precision=lax.Precision.HIGHEST, preferred_element_type=F32
        )
        g_e_gain[layer : layer + 1, :] = gains[4:5, 0:4]
        g_n_gain[layer : layer + 1, :] = gains[5:6, 0:4]


def body(
    node_latent,
    edge_latent,
    node_cotangent,
    edge_w_in,
    edge_w_out,
    node_w_in,
    node_w_out,
    edge_gain,
    node_gain,
    edge_slot,
    edge_receiver,
    send_list,
    edge_count,
):
    width = node_latent.shape[2]
    nodes = node_latent.shape[1]
    edges = edge_slot.shape[0]
    graph = lax.axis_size("graph")
    own = lax.axis_index("graph").astype(jnp.int32)
    own_arr = own.reshape(1)
    device = (own * lax.axis_size("batch") + lax.axis_index("batch").astype(jnp.int32)).reshape(1)
    slot = edge_slot.reshape(1, edges)
    receiver = edge_receiver.reshape(1, edges)
    sds = jax.ShapeDtypeStruct
    vmem = pl.BlockSpec(memory_space=pltpu.VMEM)
    smem = pl.BlockSpec(memory_space=pltpu.SMEM)
    block = sds((32, width), BF16)
    params = pltpu.CompilerParams(vmem_limit_bytes=40 * 1024 * 1024)

    weight_args = (edge_w_in, edge_w_out, node_w_in, node_w_out, edge_gain, node_gain)

    def shift(blocks, sign):
        outs = []
        for offset, value in zip(OFFSETS, blocks):
            outs.append(lax.ppermute(value, "graph", [((i + sign * offset) % graph, i) for i in range(graph)]))
        return outs

    def call(kernel, outs, scratch, specs, *args):
        return pl.pallas_call(
            kernel,
            out_shape=outs,
            in_specs=specs,
            out_specs=jax.tree.map(lambda _: vmem, outs),
            scratch_shapes=scratch,
            compiler_params=params,
        )(*args)

    onehot_s = pltpu.VMEM((512, edges), BF16)
    sender_s = pltpu.VMEM((288, width), BF16)
    proj_s = pltpu.VMEM((512, width), BF16)
    edge_b = pltpu.VMEM((edges, width), BF16)
    edge_f = pltpu.VMEM((edges, width), F32)
    grads_s = [pltpu.VMEM((r, width), BF16) for r in (1536, 512, 1024, 512)]
    half = sds((17, 112, width), BF16)
    nodes_f = sds((nodes, width), F32)
    nodes_b = sds((nodes, width), BF16)
    edges_b = sds((edges, width), BF16)
    col = sds((edges, 128), F32)

    first = call(gather_kernel, [block] * 5, [], [smem, vmem, vmem], own_arr, send_list, node_latent)
    senders0 = shift(first, 1)
    v1, vb1, eb1, pre0, normed0, inv0, n_pre0, n_normed0, n_inv0, agg0, *second = call(
        forward_kernel,
        [nodes_f, nodes_b, edges_b, edges_b, edges_b, col, nodes_f, nodes_f, sds((nodes, 128), F32), nodes_b] + [block] * 5,
        [onehot_s, sender_s, proj_s, edge_b],
        [smem, smem] + [vmem] * 10 + [vmem] * 6,
        own_arr, edge_count, send_list, slot, receiver, node_latent, edge_latent, *senders0, *weight_args,
    )
    senders1 = shift(second, 1)
    node_out, grad1, edge_grad, keep1, send1, *back1 = call(
        middle_kernel,
        [sds((1, nodes, width), F32), nodes_f, edges_b, half, half] + [block] * 5,
        [onehot_s, sender_s, proj_s, edge_b, edge_f, edge_f, pltpu.VMEM((edges, 128), F32), edge_b, edge_b, edge_b] + grads_s,
        [smem, smem] + [vmem] * 11 + [vmem] * 6,
        own_arr, edge_count, slot, receiver, v1, vb1, eb1, node_cotangent, *senders1, *weight_args,
    )

    def scatter(keep, send):
        recv = lax.ppermute(send, "graph", [(i, i ^ 1) for i in range(graph)])
        packed = call(pack_kernel, sds((64, 32, width), BF16), [pltpu.VMEM((4, 32, width), F32)], [vmem, vmem], keep, recv)
        groups = [[(2 * c + k) * 4 + b for c in range(16) for b in range(4)] for k in range(2)]
        return lax.all_to_all(packed, ("graph", "batch"), 0, 0, tiled=True, axis_index_groups=groups)

    returned1 = shift(back1, -1)
    x1 = scatter(keep1, send1)
    grad0, keep0, send0, *back0 = call(
        backward_kernel,
        [nodes_f, half, half] + [block] * 5,
        [onehot_s, sender_s, edge_b, edge_b, edge_b] + grads_s,
        [smem, smem] + [vmem] * 24 + [vmem] * 6,
        own_arr, edge_count, send_list, slot, receiver, node_latent, edge_latent, *senders0,
        grad1, *returned1, edge_grad, pre0, normed0, inv0, n_pre0, n_normed0, n_inv0, agg0, *weight_args,
    )
    returned0 = shift(back0, -1)
    x0 = scatter(keep0, send0)
    grads = call(
        finish_kernel,
        [sds((1, nodes, width), F32)] + [sds((2, r, width), F32) for r in (12, 4, 8, 4)] + [sds((2, 4), F32)] * 2,
        [pltpu.VMEM((32, width), F32)],
        [smem, smem] + [vmem] * 9,
        device, own_arr, send_list, grad0, *returned0, x0, x1,
    )
    return (node_out, *grads)


def solution(mesh):
    in_specs = (
        P("batch", "graph", None),
        P("batch", "graph", None),
        P("batch", "graph", None),
        P(),
        P(),
        P(),
        P(),
        P(),
        P(),
        P("graph"),
        P("graph"),
        P("graph", None),
        P("graph"),
    )
    out_specs = (
        P("batch", "graph", None),
        P("batch", "graph", None),
        P(None, ("graph", "batch"), None),
        P(None, ("graph", "batch"), None),
        P(None, ("graph", "batch"), None),
        P(None, ("graph", "batch"), None),
        P(None, ("graph", "batch")),
        P(None, ("graph", "batch")),
    )
    return jax.shard_map(body, mesh=mesh, in_specs=in_specs, out_specs=out_specs, check_vma=False)
```

```python
import functools

import jax
import jax.numpy as jnp
from jax import lax
from jax.experimental import pallas as pl
from jax.experimental.pallas import tpu as pltpu
from jax.sharding import PartitionSpec as P

HOPS = 2
EPSILON = 1e-05
CHUNK = 256
ORDER = (4, 2, 3, 1, 0)
F32 = jnp.float32
BF16 = jnp.bfloat16


def nn(a, b):
    return lax.dot_general(a, b, (((1,), (0,)), ((), ())), preferred_element_type=F32)


def nt(a, b):
    return lax.dot_general(a, b, (((1,), (1,)), ((), ())), preferred_element_type=F32)


def tn(a, b):
    return lax.dot_general(a, b, (((0,), (0,)), ((), ())), preferred_element_type=F32)


def sigmoid(x):
    return 0.5 * jnp.tanh(0.5 * x) + 0.5


def layer_norm(z):
    centre = z - jnp.mean(z, axis=-1, keepdims=True)
    inv = lax.rsqrt(jnp.mean(centre * centre, axis=-1, keepdims=True) + EPSILON)
    return centre * inv, inv


def layer_norm_back(grad, gain, normed, inv):
    gn = grad * gain
    m1 = jnp.mean(gn, axis=-1, keepdims=True)
    m2 = jnp.mean(gn * normed, axis=-1, keepdims=True)
    return inv * (gn - m1 - normed * m2)


def swish_back(pre):
    s = sigmoid(pre)
    return s * (1.0 + pre * (1.0 - s))


def neighbours(own):
    return own ^ 1, ((((own - 1) & 31) ^ 1) + 1) & 31, (own - 2) & 31, (own + 2) & 31, own ^ 16


def readers(own):
    swap, near, below, above, far = neighbours(own)
    return swap, near, above, below, far


def list_onehot(lists_ref, reader, nodes):
    row = lists_ref[pl.ds(reader, 1), :]
    ids = lax.broadcasted_iota(jnp.int32, (nodes, row.shape[1]), 0)
    return jnp.where(ids == row, 1.0, 0.0).astype(BF16)


def send_blocks(lists_ref, own, vb, outs):
    for reader, out in zip(readers(own), outs):
        onehot = list_onehot(lists_ref, reader, vb.shape[0])
        out[...] = tn(onehot, vb).astype(BF16)


def returned(lists_ref, own, blocks):
    total = None
    for reader, block in zip(readers(own), blocks):
        term = nn(list_onehot(lists_ref, reader, 128), block[...])
        total = term if total is None else total + term
    return total


class Copies:
    def __init__(self, sems):
        self.sems, self.count = sems, 0

    def start(self, *pairs):
        handles = []
        for source, target in pairs:
            handles.append(pltpu.make_async_copy(source, target, self.sems.at[self.count]))
            self.count += 1
        for handle in handles:
            handle.start()
        return handles


def wait(handles):
    for handle in handles:
        handle.wait()


def load_weights(copies, layer, sources, targets):
    we_in, we_out, wn_in, wn_out = sources
    te_in, te_out, tn_in, tn_out = targets
    ends = copies.start((we_in.at[layer, pl.ds(512, 1024)], te_in.at[pl.ds(512, 1024)]))
    edge = copies.start((we_in.at[layer, pl.ds(0, 512)], te_in.at[pl.ds(0, 512)]), (we_out.at[layer], te_out))
    node = copies.start((wn_in.at[layer], tn_in), (wn_out.at[layer], tn_out))
    return ends, edge, node


def build_onehot(onehot_ref, slot_ref, receiver_ref, own):
    edges = slot_ref.shape[1]
    slot = slot_ref[...]
    row = slot - 128
    source = row >> 5
    block = jnp.full(source.shape, 4, jnp.int32)
    for n, other in enumerate(neighbours(own)[:4]):
        block = jnp.where(source == other, n, block)
    position = jnp.where(slot < 128, slot, 128 + block * 32 + (row & 31))
    ids = lax.broadcasted_iota(jnp.int32, (128, edges), 0)
    onehot_ref[0:128, :] = jnp.where(ids == receiver_ref[...], 1.0, 0.0).astype(BF16)
    ids = lax.broadcasted_iota(jnp.int32, (384, edges), 0)
    onehot_ref[128:512, :] = jnp.where(ids == position, 1.0, 0.0).astype(BF16)


def fill_projected(proj_ref, vb, sender_ref, w_in_ref):
    proj_ref[0:128, :] = nn(vb, w_in_ref[1024:1536, :]).astype(BF16)
    proj_ref[128:416, :] = nn(sender_ref[...], w_in_ref[512:1024, :]).astype(BF16)
    proj_ref[416:512, :] = jnp.zeros((96, 512), BF16)


def live_rows(base, count):
    rows = base + lax.broadcasted_iota(jnp.int32, (CHUNK, 1), 0)
    return jnp.where(rows < count, 1.0, 0.0).astype(F32)


def node_forward(vb, agg, w_in_ref, w_out_ref):
    pre = nn(vb, w_in_ref[0:512, :]) + nn(agg, w_in_ref[512:1024, :])
    hidden = (pre * sigmoid(pre)).astype(BF16)
    normed, inv = layer_norm(nn(hidden, w_out_ref[...]))
    return pre, hidden, normed, inv


def split_store(k, scratch_ref, keep_ref, send_ref, at, rows):
    for c in range(16):
        mine = pl.multiple_of(2 * c * rows + k * rows, 16)
        other = pl.multiple_of(2 * c * rows + (1 - k) * rows, 16)
        keep_ref[c, at : at + rows, :] = scratch_ref[pl.ds(mine, rows), :]
        send_ref[c, at : at + rows, :] = scratch_ref[pl.ds(other, rows), :]


def store_gains(edge_gain, node_gain, keep_ref, send_ref):
    pad = jnp.concatenate([edge_gain, node_gain, jnp.zeros((14, 512), F32)], axis=0).astype(BF16)
    keep_ref[16, 0:16, :] = pad
    send_ref[16, 0:16, :] = pad


def node_backward(grad, vb, agg, pre, hidden, normed, inv, w_in_ref, w_out_ref, gain, g_in_ref, g_out_ref):
    grad_gain = jnp.sum(grad * normed, axis=0, keepdims=True)
    dz = layer_norm_back(grad, gain, normed, inv).astype(BF16)
    g_out_ref[...] = tn(hidden, dz).astype(BF16)
    da = (nt(dz, w_out_ref[...]) * swish_back(pre)).astype(BF16)
    g_in_ref[0:512, :] = tn(vb, da).astype(BF16)
    g_in_ref[512:1024, :] = tn(agg, da).astype(BF16)
    return grad_gain, nt(da, w_in_ref[0:512, :]), nt(da, w_in_ref[512:1024, :])


def gather_kernel(own_ref, lists_ref, vb_ref, o0, o1, o2, o3, o4, lists, vb, sems):
    wait(Copies(sems).start((lists_ref, lists), (vb_ref.at[0], vb)))
    send_blocks(lists, own_ref[0], vb[...], (o0, o1, o2, o3, o4))


def forward_kernel(
    own_ref, count_ref, lists_ref, slot_ref, receiver_ref, vb_ref, eb_ref, b0, b1, b2, b3, b4,
    we_in_ref, we_out_ref, wn_in_ref, wn_out_ref, e_gain_ref, n_gain_ref,
    state_out, sides_out, eb_out, saved_out, inv_out, o0, o1, o2, o3, o4,
    lists, slot, receiver, eb, we_in, we_out, wn_in, wn_out, e_gain, n_gain,
    onehot, proj, message, state, sides, eb_next, saved, inv_s, sems,
):
    own, count = own_ref[0], count_ref[0]
    copies = Copies(sems)
    index = copies.start((slot_ref, slot), (receiver_ref, receiver))
    ends = copies.start((vb_ref.at[0], sides.at[pl.ds(0, 128)]))
    ends += copies.start(*[(block, sides.at[pl.ds(128 + 32 * n, 32)]) for n, block in enumerate((b0, b1, b2, b3, b4))])
    more, edge, node = load_weights(copies, 0, (we_in_ref, we_out_ref, wn_in_ref, wn_out_ref), (we_in, we_out, wn_in, wn_out))
    edge += copies.start((eb_ref.at[0], eb), (e_gain_ref, e_gain))
    node += copies.start((n_gain_ref, n_gain), (lists_ref, lists))
    wait(index)
    build_onehot(onehot, slot, receiver, own)
    wait(ends + more)
    vb = sides[0:128, :]
    fill_projected(proj, vb, sides.at[0:288], we_in)
    wait(edge)
    gain = e_gain[0:1, :]
    saves = []
    for n in range(eb.shape[0] // CHUNK):
        rows = slice(n * CHUNK, (n + 1) * CHUNK)
        part = pl.ds(n * CHUNK, CHUNK)
        latent = eb[rows, :]
        pre = nn(latent, we_in[0:512, :]) + tn(onehot[:, rows], proj[...])
        hidden = (pre * sigmoid(pre)).astype(BF16)
        normed, inv = layer_norm(nn(hidden, we_out[...]))
        m = normed * gain * live_rows(n * CHUNK, count)
        saved[0, rows, :] = pre.astype(BF16)
        saved[1, rows, :] = normed.astype(BF16)
        inv_s[rows, :] = jnp.broadcast_to(inv, (CHUNK, 128))
        message[rows, :] = m.astype(BF16)
        eb_next[rows, :] = (latent.astype(F32) + m).astype(BF16)
        saves += copies.start(
            (eb_next.at[part], eb_out.at[part]), (saved.at[0, part], saved_out.at[0, part]),
            (saved.at[1, part], saved_out.at[1, part]), (inv_s.at[part], inv_out.at[part]),
        )
    agg = nn(onehot[0:128, :], message[...]).astype(BF16)
    wait(node)
    pre, _, normed, inv = node_forward(vb, agg, wn_in, wn_out)
    v = vb.astype(F32) + normed * n_gain[0:1, :]
    state[0] = v
    state[1] = pre
    state[2] = normed
    state[3] = jnp.broadcast_to(inv, (128, 512))
    sides[288:416, :] = agg
    saves += copies.start((state, state_out), (sides, sides_out))
    send_blocks(lists, own, v.astype(BF16), (o0, o1, o2, o3, o4))
    wait(saves)


def edge_tail(onehot, senders, vb, eb, h_ref, dz_ref, da_ref, we_in, g_in, g_out, outs):
    g_out[...] = tn(h_ref[...], dz_ref[...]).astype(BF16)
    g_in[0:512, :] = tn(eb[...], da_ref[...]).astype(BF16)
    gathered = nn(onehot[0:416, :], da_ref[...]).astype(BF16)
    at_receiver = gathered[0:128, :]
    at_sender = gathered[128:416, :]
    g_in[512:1024, :] = tn(senders[...], at_sender).astype(BF16)
    g_in[1024:1536, :] = tn(vb, at_receiver).astype(BF16)
    back = nt(at_sender, we_in[512:1024, :])
    for n, out in enumerate(outs):
        out[...] = back[128 + 32 * n : 160 + 32 * n, :].astype(BF16)
    return nt(at_receiver, we_in[1024:1536, :]) + back[0:128, :]


def write_grads(k, g_in, g_out, gn_in, gn_out, edge_gain, node_gain, keep, send):
    split_store(k, g_in, keep, send, 0, 48)
    split_store(k, g_out, keep, send, 48, 16)
    split_store(k, gn_in, keep, send, 64, 32)
    split_store(k, gn_out, keep, send, 96, 16)
    store_gains(edge_gain, node_gain, keep, send)


def middle_kernel(
    own_ref, count_ref, slot_ref, receiver_ref, state_ref, eb_ref, cot_ref, b0, b1, b2, b3, b4,
    we_in_ref, we_out_ref, wn_in_ref, wn_out_ref, e_gain_ref, n_gain_ref,
    node_out, edge_grad_out, grad_out, keep, send, o0, o1, o2, o3, o4,
    slot, receiver, v, cot, eb, we_in, we_out, wn_in, wn_out, e_gain, n_gain,
    onehot, senders, proj, message, pre_s, normed_s, inv_s, hidden_s, dz_s, da_s, edge_grad, g_in, g_out, gn_in, gn_out, sems,
):
    own, count = own_ref[0], count_ref[0]
    copies = Copies(sems)
    index = copies.start((slot_ref, slot), (receiver_ref, receiver), (state_ref.at[0], v))
    ends = copies.start(*[(block, senders.at[pl.ds(128 + 32 * n, 32)]) for n, block in enumerate((b0, b1, b2, b3, b4))])
    more, edge, node = load_weights(copies, 1, (we_in_ref, we_out_ref, wn_in_ref, wn_out_ref), (we_in, we_out, wn_in, wn_out))
    edge += copies.start((eb_ref, eb), (e_gain_ref, e_gain))
    node += copies.start((n_gain_ref, n_gain), (cot_ref.at[0], cot))
    wait(index)
    build_onehot(onehot, slot, receiver, own)
    vb = v[...].astype(BF16)
    senders[0:128, :] = vb
    wait(ends + more)
    fill_projected(proj, vb, senders, we_in)
    wait(edge)
    gain = e_gain[1:2, :]
    chunks = eb.shape[0] // CHUNK
    for n in range(chunks):
        rows = slice(n * CHUNK, (n + 1) * CHUNK)
        pre = nn(eb[rows, :], we_in[0:512, :]) + tn(onehot[:, rows], proj[...])
        hidden = (pre * sigmoid(pre)).astype(BF16)
        normed, inv = layer_norm(nn(hidden, we_out[...]))
        m = normed * gain * live_rows(n * CHUNK, count)
        pre_s[rows, :] = pre
        normed_s[rows, :] = normed
        inv_s[rows, :] = jnp.broadcast_to(inv, (CHUNK, 128))
        hidden_s[rows, :] = hidden
        message[rows, :] = m.astype(BF16)
    agg = nn(onehot[0:128, :], message[...]).astype(BF16)
    wait(node)
    n_pre, n_hidden, n_normed, n_inv = node_forward(vb, agg, wn_in, wn_out)
    n_gain_row = n_gain[1:2, :]
    v[...] = v[...] + n_normed * n_gain_row
    saves = copies.start((v, node_out.at[0]))
    grad = cot[...].astype(F32)
    grad_n_gain, grad_v, grad_agg = node_backward(
        grad, vb, agg, n_pre, n_hidden, n_normed, n_inv, wn_in, wn_out, n_gain_row, gn_in, gn_out
    )
    grad_agg = grad_agg.astype(BF16)
    grad_e_gain = jnp.zeros((1, 512), F32)
    for n in range(chunks):
        rows = slice(n * CHUNK, (n + 1) * CHUNK)
        gm = tn(onehot[0:128, rows], grad_agg) * live_rows(n * CHUNK, count)
        normed = normed_s[rows, :]
        grad_e_gain += jnp.sum(gm * normed, axis=0, keepdims=True)
        dz = layer_norm_back(gm, gain, normed, inv_s[rows, 0:1]).astype(BF16)
        dz_s[rows, :] = dz
        da = (nt(dz, we_out[...]) * swish_back(pre_s[rows, :])).astype(BF16)
        da_s[rows, :] = da
        edge_grad[rows, :] = nt(da, we_in[0:512, :]).astype(BF16)
    saves += copies.start((edge_grad, edge_grad_out))
    grad_ends = edge_tail(onehot, senders, vb, eb, hidden_s, dz_s, da_s, we_in, g_in, g_out, (o0, o1, o2, o3, o4))
    grad_out[...] = grad + grad_v + grad_ends
    write_grads(own & 1, g_in, g_out, gn_in, gn_out, grad_e_gain, grad_n_gain, keep, send)
    wait(saves)


def backward_kernel(
    own_ref, count_ref, slot_ref, receiver_ref, eb_ref, grad_ref, state_ref, sides_ref, edge_grad_ref, saved_ref, inv_ref,
    we_in_ref, we_out_ref, wn_in_ref, wn_out_ref, e_gain_ref, n_gain_ref,
    grad_out, keep, send, o0, o1, o2, o3, o4,
    slot, receiver, eb, grad_s, state, sides, edge_grad, saved, inv_s, we_in, we_out, wn_in, wn_out, e_gain, n_gain,
    onehot, hidden_s, dz_s, da_s, g_in, g_out, gn_in, gn_out, sems,
):
    own, count = own_ref[0], count_ref[0]
    copies = Copies(sems)
    first = copies.start((slot_ref, slot), (receiver_ref, receiver), (grad_ref, grad_s), (state_ref.at[pl.ds(1, 3)], state))
    first += copies.start((sides_ref, sides), (n_gain_ref, n_gain), (wn_out_ref.at[0], wn_out), (wn_in_ref.at[0], wn_in))
    edge = copies.start((edge_grad_ref, edge_grad), (saved_ref, saved), (inv_ref, inv_s), (e_gain_ref, e_gain), (we_out_ref.at[0], we_out))
    last = copies.start((eb_ref.at[0], eb), (we_in_ref.at[0], we_in))
    wait(first)
    build_onehot(onehot, slot, receiver, own)
    vb = sides[0:128, :]
    grad = grad_s[...]
    n_pre = state[0]
    n_hidden = (n_pre * sigmoid(n_pre)).astype(BF16)
    grad_n_gain, grad_v, grad_agg = node_backward(
        grad, vb, sides[288:416, :], n_pre, n_hidden, state[1], state[2], wn_in, wn_out, n_gain[0:1, :], gn_in, gn_out
    )
    grad_agg = grad_agg.astype(BF16)
    wait(edge)
    gain = e_gain[0:1, :]
    grad_e_gain = jnp.zeros((1, 512), F32)
    for n in range(eb.shape[0] // CHUNK):
        rows = slice(n * CHUNK, (n + 1) * CHUNK)
        gm = tn(onehot[0:128, rows], grad_agg) + edge_grad[rows, :].astype(F32)
        gm = gm * live_rows(n * CHUNK, count)
        normed = saved[1, rows, :].astype(F32)
        grad_e_gain += jnp.sum(gm * normed, axis=0, keepdims=True)
        dz = layer_norm_back(gm, gain, normed, inv_s[rows, 0:1]).astype(BF16)
        dz_s[rows, :] = dz
        pre = saved[0, rows, :].astype(F32)
        s = sigmoid(pre)
        hidden_s[rows, :] = (pre * s).astype(BF16)
        da_s[rows, :] = (nt(dz, we_out[...]) * (s * (1.0 + pre * (1.0 - s)))).astype(BF16)
    wait(last)
    grad_ends = edge_tail(onehot, sides.at[0:288], vb, eb, hidden_s, dz_s, da_s, we_in, g_in, g_out, (o0, o1, o2, o3, o4))
    grad_out[...] = grad + grad_v + grad_ends
    write_grads(own & 1, g_in, g_out, gn_in, gn_out, grad_e_gain, grad_n_gain, keep, send)


def pack_blocks(keep_ref, recv_ref, out_ref, stage, packed, sems):
    gains = (keep_ref[16, 0:16, :].astype(F32) + recv_ref[16, 0:16, :].astype(F32))[0:8, :]
    copies = Copies(sems)
    saves = []
    for c in range(16):
        rows = keep_ref[c].astype(F32) + recv_ref[c].astype(F32)
        for b in range(4):
            stage[b, 0:12, :] = rows[12 * b : 12 * b + 12, :]
            stage[b, 12:16, :] = rows[48 + 4 * b : 52 + 4 * b, :]
            stage[b, 16:24, :] = rows[64 + 8 * b : 72 + 8 * b, :]
            stage[b, 24:28, :] = rows[96 + 4 * b : 100 + 4 * b, :]
            stage[b, 28:32, :] = gains[0:4, :]
            packed[4 * c + b] = stage[b].astype(BF16)
        saves += copies.start((packed.at[pl.ds(4 * c, 4)], out_ref.at[pl.ds(4 * c, 4)]))
    return saves


def pack_kernel(keep_ref, recv_ref, out_ref, stage, packed, sems):
    wait(pack_blocks(keep_ref, recv_ref, out_ref, stage, packed, sems))


def pack_return_kernel(own_ref, keep_ref, recv_ref, grad_ref, lists_ref, r0, r1, r2, r3, r4, out_ref, grad_out, stage, packed, lists, grad_s, sems, grad_sems):
    loads = Copies(grad_sems)
    load = loads.start((lists_ref, lists))
    saves = pack_blocks(keep_ref, recv_ref, out_ref, stage, packed, sems)
    wait(load)
    grad_s[...] = grad_ref[...] + returned(lists, own_ref[0], (r0, r1, r2, r3, r4))
    wait(saves + loads.start((grad_s, grad_out)))


def sum_blocks(x):
    def step(n, total):
        return total + x[n].astype(F32)

    return lax.fori_loop(0, 64, step, jnp.zeros((32, 512), F32), unroll=8)


def sum_kernel(x_ref, out_ref, x, sems):
    wait(Copies(sems).start((x_ref, x)))
    out_ref[...] = sum_blocks(x)


def finish_kernel(
    device_ref, own_ref, lists_ref, grad_ref, r0, r1, r2, r3, r4, x0_ref, total1_ref,
    node_grad, g_e_in, g_e_out, g_n_in, g_n_out, g_e_gain, g_n_gain,
    lists, stage, sems,
):
    wait(Copies(sems).start((lists_ref, lists)))
    node_grad[0] = grad_ref[...] + returned(lists, own_ref[0], (r0, r1, r2, r3, r4))
    picks = lax.broadcasted_iota(jnp.int32, (512, 128), 0) - 4 * device_ref[0]
    select = jnp.where(picks == lax.broadcasted_iota(jnp.int32, (512, 128), 1), 1.0, 0.0).astype(F32)
    for layer in (1, 0):
        if layer == 0:
            stage[...] = sum_blocks(x0_ref)
        else:
            stage[...] = total1_ref[...]
        g_e_in[layer] = stage[0:12, :]
        g_e_out[layer] = stage[12:16, :]
        g_n_in[layer] = stage[16:24, :]
        g_n_out[layer] = stage[24:28, :]
        gains = lax.dot_general(
            stage[24:32, :], select, (((1,), (0,)), ((), ())), precision=lax.Precision.HIGHEST, preferred_element_type=F32
        )
        g_e_gain[layer : layer + 1, :] = gains[4:5, 0:4]
        g_n_gain[layer : layer + 1, :] = gains[5:6, 0:4]


def body(
    node_latent,
    edge_latent,
    node_cotangent,
    edge_w_in,
    edge_w_out,
    node_w_in,
    node_w_out,
    edge_gain,
    node_gain,
    edge_slot,
    edge_receiver,
    send_list,
    edge_count,
):
    width = node_latent.shape[2]
    nodes = node_latent.shape[1]
    edges = edge_slot.shape[0]
    graph = lax.axis_size("graph")
    own = lax.axis_index("graph").astype(jnp.int32)
    own_arr = own.reshape(1)
    device = (own * lax.axis_size("batch") + lax.axis_index("batch").astype(jnp.int32)).reshape(1)
    slot = edge_slot.reshape(1, edges)
    receiver = edge_receiver.reshape(1, edges)
    sds = jax.ShapeDtypeStruct
    vmem = pl.BlockSpec(memory_space=pltpu.VMEM)
    smem = pl.BlockSpec(memory_space=pltpu.SMEM)
    free = pl.BlockSpec(memory_space=pl.ANY)
    hbm = pl.BlockSpec(memory_space=pltpu.HBM)

    def exchange(blocks, back):
        sources = [(readers if back else neighbours)(i) for i in range(graph)]
        outs = {}
        for n in ORDER:
            outs[n] = lax.ppermute(blocks[n], "graph", [(sources[i][n], i) for i in range(graph)])
        return [outs[n] for n in range(5)]

    def call(kernel, mib, outs, scratch, specs, args):
        shapes = [pltpu.HBM(o.shape, o.dtype) if place is hbm else o for o, place in outs]
        args = [pltpu.with_memory_space_constraint(a, pltpu.HBM) if place is hbm else a for a, place in zip(args, specs)]
        return pl.pallas_call(
            kernel,
            out_shape=shapes,
            in_specs=[free if place is hbm else place for place in specs],
            out_specs=[free if place is hbm else place for _, place in outs],
            scratch_shapes=scratch,
            compiler_params=pltpu.CompilerParams(vmem_limit_bytes=mib * 1024 * 1024),
        )(*args)

    def vb16(*shape):
        return pltpu.VMEM(shape, BF16)

    def vf32(*shape):
        return pltpu.VMEM(shape, F32)

    def sems(n):
        return pltpu.SemaphoreType.DMA((n,))

    index_s = [pltpu.VMEM((1, edges), jnp.int32)] * 2
    lists_s = pltpu.VMEM(send_list.shape, jnp.int32)
    weights_s = [vb16(*w.shape[1:]) for w in (edge_w_in, edge_w_out, node_w_in, node_w_out)] + [vf32(*edge_gain.shape), vf32(*node_gain.shape)]
    weight_args = (edge_w_in, edge_w_out, node_w_in, node_w_out, edge_gain, node_gain)
    edge_b, edge_f = vb16(edges, width), vf32(edges, width)
    grads_s = [vb16(r, width) for r in (1536, 512, 1024, 512)]
    blocks_out = [(sds((32, width), BF16), vmem)] * 5
    half = (sds((17, 112, width), BF16), vmem)
    node_b, node_f, inv_s = vb16(nodes, width), vf32(nodes, width), vf32(edges, 128)

    first = call(gather_kernel, 2, blocks_out, [lists_s, node_b, sems(2)], [smem, hbm, hbm], (own_arr, send_list, node_latent))
    senders0 = exchange(first, False)
    state0, sides0, eb1, saved0, inv0, *second = call(
        forward_kernel,
        24,
        [(sds((4, nodes, width), F32), hbm), (sds((416, width), BF16), hbm), (sds((edges, width), BF16), hbm), (sds((2, edges, width), BF16), hbm), (sds((edges, 128), F32), hbm)] + blocks_out,
        [lists_s] + index_s + [edge_b] + weights_s + [vb16(512, edges), vb16(512, width), edge_b, vf32(4, nodes, width), vb16(416, width), edge_b, vb16(2, edges, width), inv_s, sems(48)],
        [smem, smem] + [hbm] * 5 + [free] * 5 + [hbm] * 6,
        (own_arr, edge_count, send_list, slot, receiver, node_latent, edge_latent, *senders0, *weight_args),
    )
    senders1 = exchange(second, False)
    node_out, edge_grad, grad1, keep1, send1, *back1 = call(
        middle_kernel,
        32,
        [(sds((1, nodes, width), F32), hbm), (sds((edges, width), BF16), hbm), (sds((nodes, width), F32), vmem), half, half] + blocks_out,
        index_s + [node_f, node_b, edge_b] + weights_s + [vb16(512, edges), vb16(288, width), vb16(512, width), edge_b, edge_f, edge_f, inv_s, edge_b, edge_b, edge_b, edge_b] + grads_s + [sems(24)],
        [smem, smem] + [hbm] * 5 + [free] * 5 + [hbm] * 6,
        (own_arr, edge_count, slot, receiver, state0, eb1, node_cotangent, *senders1, *weight_args),
    )

    def swap(send):
        return lax.ppermute(send, "graph", [(i, i ^ 1) for i in range(graph)])

    def spread(packed):
        groups = [[(2 * c + k) * 4 + b for c in range(16) for b in range(4)] for k in range(2)]
        return lax.all_to_all(packed, ("graph", "batch"), 0, 0, tiled=True, axis_index_groups=groups)

    packed_out = (sds((64, 32, width), BF16), hbm)
    pack_s = [vf32(4, 32, width), vb16(64, 32, width)]
    returned1 = exchange(back1, True)
    packed1, grad1 = call(
        pack_return_kernel,
        6,
        [packed_out, (sds((nodes, width), F32), hbm)],
        pack_s + [lists_s, node_f, sems(16), sems(2)],
        [smem, vmem, vmem, vmem, hbm] + [vmem] * 5,
        (own_arr, keep1, swap(send1), grad1, send_list, *returned1),
    )
    x1 = spread(packed1)
    grad0, keep0, send0, *back0 = call(
        backward_kernel,
        24,
        [(sds((nodes, width), F32), vmem), half, half] + blocks_out,
        index_s + [edge_b, node_f, vf32(3, nodes, width), vb16(416, width), edge_b, vb16(2, edges, width), inv_s] + weights_s + [vb16(512, edges), edge_b, edge_b, edge_b] + grads_s + [sems(24)],
        [smem, smem] + [hbm] * 15,
        (own_arr, edge_count, slot, receiver, edge_latent, grad1, state0, sides0, edge_grad, saved0, inv0, *weight_args),
    )
    returned0 = exchange(back0, True)
    (packed0,) = call(pack_kernel, 6, [packed_out], pack_s + [sems(16)], [vmem, vmem], (keep0, swap(send0)))
    x0 = spread(packed0)
    (total1,) = call(sum_kernel, 4, [(sds((32, width), F32), vmem)], [vb16(64, 32, width), sems(1)], [free], (x1,))
    grads = call(
        finish_kernel,
        6,
        [(sds((1, nodes, width), F32), vmem)] + [(sds((2, r, width), F32), vmem) for r in (12, 4, 8, 4)] + [(sds((2, 4), F32), vmem)] * 2,
        [lists_s, vf32(32, width), sems(1)],
        [smem, smem, hbm] + [vmem] * 8,
        (device, own_arr, send_list, grad0, *returned0, x0, total1),
    )
    return (node_out, *grads)


def solution(mesh):
    in_specs = (
        P("batch", "graph", None),
        P("batch", "graph", None),
        P("batch", "graph", None),
        P(),
        P(),
        P(),
        P(),
        P(),
        P(),
        P("graph"),
        P("graph"),
        P("graph", None),
        P("graph"),
    )
    out_specs = (
        P("batch", "graph", None),
        P("batch", "graph", None),
        P(None, ("graph", "batch"), None),
        P(None, ("graph", "batch"), None),
        P(None, ("graph", "batch"), None),
        P(None, ("graph", "batch"), None),
        P(None, ("graph", "batch")),
        P(None, ("graph", "batch")),
    )
    return jax.shard_map(body, mesh=mesh, in_specs=in_specs, out_specs=out_specs, check_vma=False)
```

```python
import jax
import jax.numpy as jnp
from jax import lax
from jax.experimental import pallas as pl
from jax.experimental.pallas import tpu as pltpu
from jax.sharding import PartitionSpec as P


EPSILON = 1e-05
CHUNK = 256
ORDER = (4, 2, 3, 1, 0)
F32 = jnp.float32
BF16 = jnp.bfloat16


def nn(a, b):
    return lax.dot_general(a, b, (((1,), (0,)), ((), ())), preferred_element_type=F32)


def nt(a, b):
    return lax.dot_general(a, b, (((1,), (1,)), ((), ())), preferred_element_type=F32)


def tn(a, b):
    return lax.dot_general(a, b, (((0,), (0,)), ((), ())), preferred_element_type=F32)


def sigmoid(x):
    return 0.5 * jnp.tanh(0.5 * x) + 0.5


def layer_norm(z):
    centre = z - jnp.mean(z, axis=-1, keepdims=True)
    inv = lax.rsqrt(jnp.mean(centre * centre, axis=-1, keepdims=True) + EPSILON)
    return centre * inv, inv


def layer_norm_back(grad, gain, normed, inv):
    gn = grad * gain
    m1 = jnp.mean(gn, axis=-1, keepdims=True)
    m2 = jnp.mean(gn * normed, axis=-1, keepdims=True)
    return inv * (gn - m1 - normed * m2)


def swish_back(pre):
    s = sigmoid(pre)
    return s * (1.0 + pre * (1.0 - s))


def neighbours(own):
    return own ^ 1, ((((own - 1) & 31) ^ 1) + 1) & 31, (own - 2) & 31, (own + 2) & 31, own ^ 16


def readers(own):
    swap, near, below, above, far = neighbours(own)
    return swap, near, above, below, far


def list_onehot(lists_ref, reader, nodes):
    row = lists_ref[pl.ds(reader, 1), :]
    ids = lax.broadcasted_iota(jnp.int32, (nodes, row.shape[1]), 0)
    return jnp.where(ids == row, 1.0, 0.0).astype(BF16)


def send_blocks(lists_ref, own, vb, outs):
    for reader, out in zip(readers(own), outs):
        onehot = list_onehot(lists_ref, reader, vb.shape[0])
        out[...] = tn(onehot, vb).astype(BF16)


def returned(lists_ref, own, blocks):
    total = None
    for reader, block in zip(readers(own), blocks):
        term = nn(list_onehot(lists_ref, reader, 128), block[...])
        total = term if total is None else total + term
    return total


class Copies:
    def __init__(self, sems):
        self.sems, self.count = sems, 0

    def start(self, *pairs):
        handles = []
        for source, target in pairs:
            handles.append(pltpu.make_async_copy(source, target, self.sems.at[self.count]))
            self.count += 1
        for handle in handles:
            handle.start()
        return handles


def wait(handles):
    for handle in handles:
        handle.wait()


def build_onehot(onehot_ref, slot_ref, receiver_ref, own):
    edges = slot_ref.shape[1]
    slot = slot_ref[...]
    row = slot - 128
    source = row >> 5
    block = jnp.full(source.shape, 4, jnp.int32)
    for n, other in enumerate(neighbours(own)[:4]):
        block = jnp.where(source == other, n, block)
    position = jnp.where(slot < 128, slot, 128 + block * 32 + (row & 31))
    ids = lax.broadcasted_iota(jnp.int32, (128, edges), 0)
    onehot_ref[0:128, :] = jnp.where(ids == receiver_ref[...], 1.0, 0.0).astype(BF16)
    ids = lax.broadcasted_iota(jnp.int32, (384, edges), 0)
    onehot_ref[128:512, :] = jnp.where(ids == position, 1.0, 0.0).astype(BF16)


def live_rows(base, count):
    rows = base + lax.broadcasted_iota(jnp.int32, (CHUNK, 1), 0)
    return jnp.where(rows < count, 1.0, 0.0).astype(F32)


def node_forward(vb, agg, w_in_ref, w_out_ref):
    pre = nn(vb, w_in_ref[0:512, :]) + nn(agg, w_in_ref[512:1024, :])
    hidden = (pre * sigmoid(pre)).astype(BF16)
    normed, inv = layer_norm(nn(hidden, w_out_ref[...]))
    return pre, hidden, normed, inv


def split_store(k, scratch_ref, keep_ref, send_ref, at, rows):
    for c in range(16):
        mine = pl.multiple_of(2 * c * rows + k * rows, 16)
        other = pl.multiple_of(2 * c * rows + (1 - k) * rows, 16)
        keep_ref[c, at : at + rows, :] = scratch_ref[pl.ds(mine, rows), :]
        send_ref[c, at : at + rows, :] = scratch_ref[pl.ds(other, rows), :]


def store_gains(edge_gain, node_gain, keep_ref, send_ref):
    pad = jnp.concatenate([edge_gain, node_gain, jnp.zeros((14, 512), F32)], axis=0).astype(BF16)
    keep_ref[16, 0:16, :] = pad
    send_ref[16, 0:16, :] = pad


def node_backward(grad, vb, agg, pre, hidden, normed, inv, w_in_ref, w_out_ref, gain, g_in_ref, g_out_ref):
    grad_gain = jnp.sum(grad * normed, axis=0, keepdims=True)
    dz = layer_norm_back(grad, gain, normed, inv).astype(BF16)
    g_out_ref[...] = tn(hidden, dz).astype(BF16)
    da = (nt(dz, w_out_ref[...]) * swish_back(pre)).astype(BF16)
    g_in_ref[0:512, :] = tn(vb, da).astype(BF16)
    g_in_ref[512:1024, :] = tn(agg, da).astype(BF16)
    return grad_gain, nt(da, w_in_ref[0:512, :]), nt(da, w_in_ref[512:1024, :])


def gather_kernel(own_ref, lists_ref, vb_ref, lists, vb, o0, o1, o2, o3, o4, sems):
    wait(Copies(sems).start((lists_ref, lists), (vb_ref.at[0], vb)))
    send_blocks(lists, own_ref[0], vb[...], (o0, o1, o2, o3, o4))


def start_weights(copies, layer, sources, targets):
    return [copies.start((source.at[layer], target)) for source, target in zip(sources, targets)]


def first_kernel(
    own_ref, slot_ref, receiver_ref, eb_ref, vb, we_in_ref, we_out_ref, wn_in_ref, wn_out_ref, e_gain_ref, n_gain_ref,
    onehot, eb, we_in, we_out, wn_in, wn_out, e_gain, n_gain, part, proj,
    slot, receiver, sems,
):
    copies = Copies(sems)
    index = copies.start((slot_ref, slot), (receiver_ref, receiver))
    loads = start_weights(copies, 0, (we_in_ref, we_out_ref, wn_in_ref, wn_out_ref), (we_in, we_out, wn_in, wn_out))
    latent = copies.start((eb_ref.at[0], eb))
    gains = copies.start((e_gain_ref, e_gain), (n_gain_ref, n_gain))
    wait(index)
    build_onehot(onehot, slot, receiver, own_ref[0])
    wait(loads[0])
    proj[0:128, :] = nn(vb[...], we_in[1024:1536, :]).astype(BF16)
    proj[128:256, :] = nn(vb[...], we_in[512:1024, :]).astype(BF16)
    wait(latent)
    part[...] = nn(eb[...], we_in[0:512, :])
    for load in loads[1:]:
        wait(load)
    wait(gains)


def second_kernel(
    state, eb, cot_ref, we_in_ref, we_out_ref, wn_in_ref, wn_out_ref,
    cot, we_in, we_out, wn_in, wn_out, part, proj, sems,
):
    copies = Copies(sems)
    loads = start_weights(copies, 1, (we_in_ref, we_out_ref, wn_in_ref, wn_out_ref), (we_in, we_out, wn_in, wn_out))
    load = copies.start((cot_ref.at[0], cot))
    vb = state[0].astype(BF16)
    wait(loads[0])
    proj[0:128, :] = nn(vb, we_in[1024:1536, :]).astype(BF16)
    proj[128:256, :] = nn(vb, we_in[512:1024, :]).astype(BF16)
    part[...] = nn(eb[...], we_in[0:512, :])
    for handles in loads[1:]:
        wait(handles)
    wait(load)


def fill_remote(proj, near, senders, vb, blocks, w_in_ref):
    senders[0:128, :] = vb
    for n, block in enumerate(blocks):
        senders[128 + 32 * n : 160 + 32 * n, :] = block[...]
    proj[0:256, :] = near[...]
    proj[256:416, :] = nn(senders[128:288, :], w_in_ref[512:1024, :]).astype(BF16)
    proj[416:512, :] = jnp.zeros((96, 512), BF16)


def forward_kernel(
    own_ref, count_ref, lists, vb_ref, onehot, eb, we_in, we_out, wn_in, wn_out, e_gain, n_gain, part, near, b0, b1, b2, b3, b4,
    state, sides, eb_next, saved_out, inv_out, o0, o1, o2, o3, o4,
    proj, message, saved, inv_s, sems,
):
    own, count = own_ref[0], count_ref[0]
    vb = vb_ref[...]
    fill_remote(proj, near, sides, vb, (b0, b1, b2, b3, b4), we_in)
    gain = e_gain[0:1, :]
    copies, saves = Copies(sems), []
    for n in range(eb.shape[0] // CHUNK):
        rows = slice(n * CHUNK, (n + 1) * CHUNK)
        pre = part[rows, :] + tn(onehot[:, rows], proj[...])
        hidden = (pre * sigmoid(pre)).astype(BF16)
        normed, inv = layer_norm(nn(hidden, we_out[...]))
        m = normed * gain * live_rows(n * CHUNK, count)
        saved[0, rows, :] = pre.astype(BF16)
        saved[1, rows, :] = normed.astype(BF16)
        inv_s[rows, :] = jnp.broadcast_to(inv, (CHUNK, 128))
        message[rows, :] = m.astype(BF16)
        eb_next[rows, :] = (eb[rows, :].astype(F32) + m).astype(BF16)
        at = pl.ds(n * CHUNK, CHUNK)
        saves += copies.start(
            (saved.at[0, at], saved_out.at[0, at]), (saved.at[1, at], saved_out.at[1, at]), (inv_s.at[at], inv_out.at[at])
        )
    agg = nn(onehot[0:128, :], message[...]).astype(BF16)
    pre, _, normed, inv = node_forward(vb, agg, wn_in, wn_out)
    v = vb.astype(F32) + normed * n_gain[0:1, :]
    state[0] = v
    state[1] = pre
    state[2] = normed
    state[3] = jnp.broadcast_to(inv, (128, 512))
    sides[288:416, :] = agg
    send_blocks(lists, own, v.astype(BF16), (o0, o1, o2, o3, o4))
    wait(saves)


def edge_tail(onehot, senders, vb, eb, h_ref, dz_ref, da_ref, we_in, g_in, g_out, outs):
    g_out[...] = tn(h_ref[...], dz_ref[...]).astype(BF16)
    g_in[0:512, :] = tn(eb[...], da_ref[...]).astype(BF16)
    gathered = nn(onehot[0:416, :], da_ref[...]).astype(BF16)
    at_receiver = gathered[0:128, :]
    at_sender = gathered[128:416, :]
    g_in[512:1024, :] = tn(senders[...], at_sender).astype(BF16)
    g_in[1024:1536, :] = tn(vb, at_receiver).astype(BF16)
    back = nt(at_sender, we_in[512:1024, :])
    for n, out in enumerate(outs):
        out[...] = back[128 + 32 * n : 160 + 32 * n, :].astype(BF16)
    return nt(at_receiver, we_in[1024:1536, :]) + back[0:128, :]


def write_grads(k, g_in, g_out, gn_in, gn_out, edge_gain, node_gain, keep, send):
    split_store(k, g_in, keep, send, 0, 48)
    split_store(k, g_out, keep, send, 48, 16)
    split_store(k, gn_in, keep, send, 64, 32)
    split_store(k, gn_out, keep, send, 96, 16)
    store_gains(edge_gain, node_gain, keep, send)


def middle_kernel(
    own_ref, count_ref, state, onehot, eb, cot, we_in, we_out, wn_in, wn_out, e_gain, n_gain, part, near, b0, b1, b2, b3, b4,
    node_out, edge_grad_out, grad_out, keep, send, o0, o1, o2, o3, o4,
    v, edge_grad, senders, proj, message, pre_s, normed_s, inv_s, hidden_s, dz_s, da_s, g_in, g_out, gn_in, gn_out, sems,
):
    own, count = own_ref[0], count_ref[0]
    vb = state[0].astype(BF16)
    fill_remote(proj, near, senders, vb, (b0, b1, b2, b3, b4), we_in)
    gain = e_gain[1:2, :]
    chunks = eb.shape[0] // CHUNK
    for n in range(chunks):
        rows = slice(n * CHUNK, (n + 1) * CHUNK)
        pre = part[rows, :] + tn(onehot[:, rows], proj[...])
        hidden = (pre * sigmoid(pre)).astype(BF16)
        normed, inv = layer_norm(nn(hidden, we_out[...]))
        m = normed * gain * live_rows(n * CHUNK, count)
        pre_s[rows, :] = pre
        normed_s[rows, :] = normed
        inv_s[rows, :] = jnp.broadcast_to(inv, (CHUNK, 128))
        hidden_s[rows, :] = hidden
        message[rows, :] = m.astype(BF16)
    agg = nn(onehot[0:128, :], message[...]).astype(BF16)
    n_pre, n_hidden, n_normed, n_inv = node_forward(vb, agg, wn_in, wn_out)
    n_gain_row = n_gain[1:2, :]
    v[...] = state[0] + n_normed * n_gain_row
    copies = Copies(sems)
    saves = copies.start((v, node_out.at[0]))
    grad = cot[...].astype(F32)
    grad_n_gain, grad_v, grad_agg = node_backward(
        grad, vb, agg, n_pre, n_hidden, n_normed, n_inv, wn_in, wn_out, n_gain_row, gn_in, gn_out
    )
    grad_agg = grad_agg.astype(BF16)
    grad_e_gain = jnp.zeros((1, 512), F32)
    for n in range(chunks):
        rows = slice(n * CHUNK, (n + 1) * CHUNK)
        gm = tn(onehot[0:128, rows], grad_agg) * live_rows(n * CHUNK, count)
        normed = normed_s[rows, :]
        grad_e_gain += jnp.sum(gm * normed, axis=0, keepdims=True)
        dz = layer_norm_back(gm, gain, normed, inv_s[rows, 0:1]).astype(BF16)
        dz_s[rows, :] = dz
        da = (nt(dz, we_out[...]) * swish_back(pre_s[rows, :])).astype(BF16)
        da_s[rows, :] = da
        edge_grad[rows, :] = nt(da, we_in[0:512, :]).astype(BF16)
        at = pl.ds(n * CHUNK, CHUNK)
        saves += copies.start((edge_grad.at[at], edge_grad_out.at[at]))
    grad_ends = edge_tail(onehot, senders, vb, eb, hidden_s, dz_s, da_s, we_in, g_in, g_out, (o0, o1, o2, o3, o4))
    grad_out[...] = grad + grad_v + grad_ends
    write_grads(own & 1, g_in, g_out, gn_in, gn_out, grad_e_gain, grad_n_gain, keep, send)
    wait(saves)


def backward_kernel(
    own_ref, count_ref, lists, onehot, grad_ref, r0, r1, r2, r3, r4, eb_ref, state_ref, sides_ref, edge_grad_ref, saved_ref, inv_ref,
    we_in_ref, we_out_ref, wn_in_ref, wn_out_ref, e_gain_ref, n_gain_ref,
    grad_out, keep, send, o0, o1, o2, o3, o4,
    eb, state, sides, edge_grad, saved, inv_s, we_in, we_out, wn_in, wn_out, e_gain, n_gain,
    hidden_s, dz_s, da_s, g_in, g_out, gn_in, gn_out, sems,
):
    own, count = own_ref[0], count_ref[0]
    copies = Copies(sems)
    node = copies.start((state_ref.at[pl.ds(1, 3)], state), (sides_ref, sides), (n_gain_ref, n_gain))
    node += copies.start((wn_out_ref.at[0], wn_out), (wn_in_ref.at[0], wn_in))
    edge = copies.start((edge_grad_ref, edge_grad), (saved_ref, saved), (inv_ref, inv_s), (e_gain_ref, e_gain), (we_out_ref.at[0], we_out))
    last = copies.start((eb_ref.at[0], eb), (we_in_ref.at[0], we_in))
    wait(node)
    vb = sides[0:128, :]
    grad = grad_ref[...] + returned(lists, own, (r0, r1, r2, r3, r4))
    n_pre = state[0]
    n_hidden = (n_pre * sigmoid(n_pre)).astype(BF16)
    grad_n_gain, grad_v, grad_agg = node_backward(
        grad, vb, sides[288:416, :], n_pre, n_hidden, state[1], state[2], wn_in, wn_out, n_gain[0:1, :], gn_in, gn_out
    )
    grad_agg = grad_agg.astype(BF16)
    wait(edge)
    gain = e_gain[0:1, :]
    grad_e_gain = jnp.zeros((1, 512), F32)
    for n in range(eb.shape[0] // CHUNK):
        rows = slice(n * CHUNK, (n + 1) * CHUNK)
        gm = tn(onehot[0:128, rows], grad_agg) + edge_grad[rows, :].astype(F32)
        gm = gm * live_rows(n * CHUNK, count)
        normed = saved[1, rows, :].astype(F32)
        grad_e_gain += jnp.sum(gm * normed, axis=0, keepdims=True)
        dz = layer_norm_back(gm, gain, normed, inv_s[rows, 0:1]).astype(BF16)
        dz_s[rows, :] = dz
        pre = saved[0, rows, :].astype(F32)
        s = sigmoid(pre)
        hidden_s[rows, :] = (pre * s).astype(BF16)
        da_s[rows, :] = (nt(dz, we_out[...]) * (s * (1.0 + pre * (1.0 - s)))).astype(BF16)
    wait(last)
    grad_ends = edge_tail(onehot, sides.at[0:288], vb, eb, hidden_s, dz_s, da_s, we_in, g_in, g_out, (o0, o1, o2, o3, o4))
    grad_out[...] = grad + grad_v + grad_ends
    write_grads(own & 1, g_in, g_out, gn_in, gn_out, grad_e_gain, grad_n_gain, keep, send)


def pack_blocks(keep_ref, recv_ref, out_ref, stage, packed, sems):
    gains = (keep_ref[16, 0:16, :].astype(F32) + recv_ref[16, 0:16, :].astype(F32))[0:8, :]
    copies = Copies(sems)
    saves = []
    for c in range(16):
        rows = keep_ref[c].astype(F32) + recv_ref[c].astype(F32)
        for b in range(4):
            stage[b, 0:12, :] = rows[12 * b : 12 * b + 12, :]
            stage[b, 12:16, :] = rows[48 + 4 * b : 52 + 4 * b, :]
            stage[b, 16:24, :] = rows[64 + 8 * b : 72 + 8 * b, :]
            stage[b, 24:28, :] = rows[96 + 4 * b : 100 + 4 * b, :]
            stage[b, 28:32, :] = gains[0:4, :]
            packed[4 * c + b] = stage[b].astype(BF16)
        saves += copies.start((packed.at[pl.ds(4 * c, 4)], out_ref.at[pl.ds(4 * c, 4)]))
    return saves


def pack_kernel(keep_ref, recv_ref, out_ref, stage, packed, sems):
    wait(pack_blocks(keep_ref, recv_ref, out_ref, stage, packed, sems))


def sum_blocks(x):
    def step(n, total):
        return total + x[n].astype(F32)

    return lax.fori_loop(0, 64, step, jnp.zeros((32, 512), F32), unroll=8)


def pick_gains(rows, device):
    picks = lax.broadcasted_iota(jnp.int32, (512, 128), 0) - 4 * device
    select = jnp.where(picks == lax.broadcasted_iota(jnp.int32, (512, 128), 1), 1.0, 0.0).astype(F32)
    return lax.dot_general(rows, select, (((1,), (0,)), ((), ())), precision=lax.Precision.HIGHEST, preferred_element_type=F32)


def sum_kernel(device_ref, x_ref, out_ref, gains_ref, x, sems):
    wait(Copies(sems).start((x_ref, x)))
    out_ref[...] = sum_blocks(x)
    gains_ref[...] = pick_gains(out_ref[24:32, :], device_ref[0])


def node_grad_kernel(own_ref, lists, grad_ref, r0, r1, r2, r3, r4, out_ref, total, sems):
    total[...] = grad_ref[...] + returned(lists, own_ref[0], (r0, r1, r2, r3, r4))
    wait(Copies(sems).start((total, out_ref.at[0])))


def finish_kernel(device_ref, x0_ref, total1, gains1, g_e_in, g_e_out, g_n_in, g_n_out, g_e_gain, g_n_gain, total0):
    total0[...] = sum_blocks(x0_ref)
    for layer, total in ((0, total0), (1, total1)):
        g_e_in[:, layer, :] = total[0:12, :]
        g_e_out[layer] = total[12:16, :]
        g_n_in[layer] = total[16:24, :]
        g_n_out[layer] = total[24:28, :]
        gains = gains1[...] if layer else pick_gains(total[24:32, :], device_ref[0])
        g_e_gain[layer : layer + 1, :] = gains[4:5, 0:4]
        g_n_gain[layer : layer + 1, :] = gains[5:6, 0:4]


def body(
    node_latent,
    edge_latent,
    node_cotangent,
    edge_w_in,
    edge_w_out,
    node_w_in,
    node_w_out,
    edge_gain,
    node_gain,
    edge_slot,
    edge_receiver,
    send_list,
    edge_count,
):
    width = node_latent.shape[2]
    nodes = node_latent.shape[1]
    edges = edge_slot.shape[0]
    graph = lax.axis_size("graph")
    own = lax.axis_index("graph").astype(jnp.int32)
    own_arr = own.reshape(1)
    device = (own * lax.axis_size("batch") + lax.axis_index("batch").astype(jnp.int32)).reshape(1)
    slot = edge_slot.reshape(1, edges)
    receiver = edge_receiver.reshape(1, edges)
    sds = jax.ShapeDtypeStruct
    vmem = pl.BlockSpec(memory_space=pltpu.VMEM)
    smem = pl.BlockSpec(memory_space=pltpu.SMEM)
    free = pl.BlockSpec(memory_space=pl.ANY)
    hbm = pl.BlockSpec(memory_space=pltpu.HBM)
    kept = pl.BlockSpec(memory_space=pltpu.VMEM)

    def exchange(blocks, back):
        sources = [(readers if back else neighbours)(i) for i in range(graph)]
        outs = {}
        for n in ORDER:
            outs[n] = lax.ppermute(blocks[n], "graph", [(sources[i][n], i) for i in range(graph)])
        return [outs[n] for n in range(5)]

    def call(kernel, mib, outs, scratch, specs, args):
        at = {id(hbm): pltpu.HBM, id(kept): pltpu.VMEM}
        real = {id(hbm): free, id(kept): vmem}
        shapes = [at[id(p)](o.shape, o.dtype) if id(p) in at else o for o, p in outs]
        args = [pltpu.with_memory_space_constraint(a, at[id(p)]) if id(p) in at else a for a, p in zip(args, specs)]
        return pl.pallas_call(
            kernel,
            out_shape=shapes,
            in_specs=[real.get(id(p), p) for p in specs],
            out_specs=[real.get(id(p), p) for _, p in outs],
            scratch_shapes=scratch,
            compiler_params=pltpu.CompilerParams(vmem_limit_bytes=mib * 1024 * 1024),
        )(*args)

    def vb16(*shape):
        return pltpu.VMEM(shape, BF16)

    def vf32(*shape):
        return pltpu.VMEM(shape, F32)

    def sems(n):
        return pltpu.SemaphoreType.DMA((n,))

    def ob16(*shape):
        return (sds(shape, BF16), kept)

    def of32(*shape):
        return (sds(shape, F32), kept)

    def swap(send):
        return lax.ppermute(send, "graph", [(i, i ^ 1) for i in range(graph)])

    def spread(packed):
        groups = [[(2 * c + k) * 4 + b for c in range(16) for b in range(4)] for k in range(2)]
        return lax.all_to_all(packed, ("graph", "batch"), 0, 0, tiled=True, axis_index_groups=groups)

    index_s = [pltpu.VMEM((1, edges), jnp.int32)] * 2
    weights = (edge_w_in, edge_w_out, node_w_in, node_w_out)
    weights_s = [vb16(*w.shape[1:]) for w in weights] + [vf32(*edge_gain.shape), vf32(*node_gain.shape)]
    weights_out = [ob16(*w.shape[1:]) for w in weights]
    edge_b, edge_f = vb16(edges, width), vf32(edges, width)
    grads_s = [vb16(r, width) for r in (1536, 512, 1024, 512)]
    blocks_out = [(sds((32, width), BF16), vmem)] * 5
    half = (sds((17, 112, width), BF16), vmem)

    lists, vb0, *first = call(
        gather_kernel, 2, [(sds(send_list.shape, jnp.int32), kept), ob16(nodes, width)] + blocks_out, [sems(2)],
        [smem, hbm, hbm], (own_arr, send_list, node_latent),
    )
    senders0 = exchange(first, False)
    onehot, eb0, we_in0, we_out0, wn_in0, wn_out0, e_gain, n_gain, part0, near0 = call(
        first_kernel,
        4,
        [ob16(512, edges), ob16(edges, width)] + weights_out + [of32(*edge_gain.shape), of32(*node_gain.shape), of32(edges, width), ob16(256, width)],
        index_s + [sems(12)],
        [smem, hbm, hbm, hbm, kept] + [hbm] * 6,
        (own_arr, slot, receiver, edge_latent, vb0, *weights, edge_gain, node_gain),
    )
    weights0 = (we_in0, we_out0, wn_in0, wn_out0, e_gain, n_gain)
    state, sides, eb1, saved, inv, *second = call(
        forward_kernel,
        10,
        [of32(4, nodes, width), ob16(416, width), ob16(edges, width), (sds((2, edges, width), BF16), hbm), (sds((edges, 128), F32), hbm)] + blocks_out,
        [vb16(512, width), edge_b, vb16(2, edges, width), vf32(edges, 128), sems(16)],
        [smem, smem] + [kept] * 12 + [vmem] * 5,
        (own_arr, edge_count, lists, vb0, onehot, eb0, *weights0, part0, near0, *senders0),
    )
    senders1 = exchange(second, False)
    cot, we_in1, we_out1, wn_in1, wn_out1, part1, near1 = call(
        second_kernel,
        4,
        [ob16(nodes, width)] + weights_out + [of32(edges, width), ob16(256, width)],
        [sems(8)],
        [kept, kept] + [hbm] * 5,
        (state, eb1, node_cotangent, *weights),
    )
    node_out, edge_grad, grad1, keep1, send1, *back1 = call(
        middle_kernel,
        20,
        [(sds((1, nodes, width), F32), hbm), (sds((edges, width), BF16), hbm), of32(nodes, width), half, half] + blocks_out,
        [vf32(nodes, width), edge_b, vb16(288, width), vb16(512, width), edge_b, edge_f, edge_f, vf32(edges, 128), edge_b, edge_b, edge_b] + grads_s + [sems(8)],
        [smem, smem] + [kept] * 12 + [vmem] * 5,
        (own_arr, edge_count, state, onehot, eb1, cot, we_in1, we_out1, wn_in1, wn_out1, e_gain, n_gain, part1, near1, *senders1),
    )
    packed_out = (sds((64, 32, width), BF16), hbm)
    pack_s = [vf32(4, 32, width), vb16(64, 32, width), sems(16)]
    returned1 = exchange(back1, True)
    (packed1,) = call(pack_kernel, 5, [packed_out], pack_s, [vmem, vmem], (keep1, swap(send1)))
    x1 = spread(packed1)
    grad0, keep0, send0, *back0 = call(
        backward_kernel,
        22,
        [(sds((nodes, width), F32), vmem), half, half] + blocks_out,
        [edge_b, vf32(3, nodes, width), vb16(416, width), edge_b, vb16(2, edges, width), vf32(edges, 128)] + weights_s + [edge_b, edge_b, edge_b] + grads_s + [sems(12)],
        [smem, smem, kept, kept] + [vmem] * 6 + [hbm, free, free] + [hbm] * 9,
        (own_arr, edge_count, lists, onehot, grad1, *returned1, edge_latent, state, sides, edge_grad, saved, inv, *weights, edge_gain, node_gain),
    )
    returned0 = exchange(back0, True)
    (packed0,) = call(pack_kernel, 5, [packed_out], pack_s, [vmem, vmem], (keep0, swap(send0)))
    x0 = spread(packed0)
    total1, gains1 = call(
        sum_kernel, 4, [of32(32, width), of32(8, 128)], [vb16(64, 32, width), sems(1)], [smem, free], (device, x1)
    )
    (node_grad,) = call(
        node_grad_kernel, 2, [(sds((1, nodes, width), F32), hbm)], [vf32(nodes, width), sems(1)],
        [smem, kept, vmem] + [vmem] * 5, (own_arr, lists, grad0, *returned0),
    )
    g_e_in, *grads = call(
        finish_kernel,
        2,
        [(sds((12, 2, width), F32), vmem)] + [(sds((2, r, width), F32), vmem) for r in (4, 8, 4)] + [(sds((2, 4), F32), vmem)] * 2,
        [vf32(32, width)],
        [smem, vmem, kept, kept],
        (device, x0, total1, gains1),
    )
    return (node_out, node_grad, jnp.swapaxes(g_e_in, 0, 1), *grads)


def solution(mesh):
    in_specs = (
        P("batch", "graph", None),
        P("batch", "graph", None),
        P("batch", "graph", None),
        P(),
        P(),
        P(),
        P(),
        P(),
        P(),
        P("graph"),
        P("graph"),
        P("graph", None),
        P("graph"),
    )
    out_specs = (
        P("batch", "graph", None),
        P("batch", "graph", None),
        P(None, ("graph", "batch"), None),
        P(None, ("graph", "batch"), None),
        P(None, ("graph", "batch"), None),
        P(None, ("graph", "batch"), None),
        P(None, ("graph", "batch")),
        P(None, ("graph", "batch")),
    )
    return jax.shard_map(body, mesh=mesh, in_specs=in_specs, out_specs=out_specs, check_vma=False)
```

```python
import jax
import jax.numpy as jnp
from jax import lax
from jax.experimental import pallas as pl
from jax.experimental.pallas import tpu as pltpu
from jax.sharding import PartitionSpec as P


EPSILON = 1e-05
CHUNK = 512
ORDER = (4, 2, 3, 1, 0)
F32 = jnp.float32
BF16 = jnp.bfloat16


def nn(a, b):
    return lax.dot_general(a, b, (((1,), (0,)), ((), ())), preferred_element_type=F32)


def nt(a, b):
    return lax.dot_general(a, b, (((1,), (1,)), ((), ())), preferred_element_type=F32)


def tn(a, b):
    return lax.dot_general(a, b, (((0,), (0,)), ((), ())), preferred_element_type=F32)


def sigmoid(x):
    return 0.5 * jnp.tanh(0.5 * x) + 0.5


def layer_norm(z):
    centre = z - jnp.mean(z, axis=-1, keepdims=True)
    inv = lax.rsqrt(jnp.mean(centre * centre, axis=-1, keepdims=True) + EPSILON)
    return centre * inv, inv


def layer_norm_back(grad, gain, normed, inv):
    gn = grad * gain
    m1 = jnp.mean(gn, axis=-1, keepdims=True)
    m2 = jnp.mean(gn * normed, axis=-1, keepdims=True)
    return inv * (gn - m1 - normed * m2)


def swish_back(pre):
    s = sigmoid(pre)
    return s * (1.0 + pre * (1.0 - s))


def neighbours(own):
    return own ^ 1, ((((own - 1) & 31) ^ 1) + 1) & 31, (own - 2) & 31, (own + 2) & 31, own ^ 16


def readers(own):
    swap, near, below, above, far = neighbours(own)
    return swap, near, above, below, far


def list_onehot(lists_ref, reader, nodes):
    row = lists_ref[pl.ds(reader, 1), :]
    ids = lax.broadcasted_iota(jnp.int32, (nodes, row.shape[1]), 0)
    return jnp.where(ids == row, 1.0, 0.0).astype(BF16)


def send_blocks(lists_ref, own, vb, outs):
    for reader, out in zip(readers(own), outs):
        onehot = list_onehot(lists_ref, reader, vb.shape[0])
        out[...] = tn(onehot, vb).astype(BF16)


def returned(lists_ref, own, blocks):
    total = None
    for reader, block in zip(readers(own), blocks):
        term = nn(list_onehot(lists_ref, reader, 128), block[...])
        total = term if total is None else total + term
    return total


class Copies:
    def __init__(self, sems):
        self.sems, self.count = sems, 0

    def start(self, *pairs):
        handles = []
        for source, target in pairs:
            handles.append(pltpu.make_async_copy(source, target, self.sems.at[self.count]))
            self.count += 1
        for handle in handles:
            handle.start()
        return handles


def wait(handles):
    for handle in handles:
        handle.wait()


def build_onehot(onehot_ref, slot_ref, receiver_ref, own):
    edges = slot_ref.shape[1]
    slot = slot_ref[...]
    row = slot - 128
    source = row >> 5
    block = jnp.full(source.shape, 4, jnp.int32)
    for n, other in enumerate(neighbours(own)[:4]):
        block = jnp.where(source == other, n, block)
    position = jnp.where(slot < 128, slot, 128 + block * 32 + (row & 31))
    ids = lax.broadcasted_iota(jnp.int32, (128, edges), 0)
    onehot_ref[0:128, :] = jnp.where(ids == receiver_ref[...], 1.0, 0.0).astype(BF16)
    ids = lax.broadcasted_iota(jnp.int32, (384, edges), 0)
    onehot_ref[128:512, :] = jnp.where(ids == position, 1.0, 0.0).astype(BF16)


def live_rows(base, count):
    rows = base + lax.broadcasted_iota(jnp.int32, (CHUNK, 1), 0)
    return jnp.where(rows < count, 1.0, 0.0).astype(F32)


def node_forward(vb, agg, w_in_ref, w_out_ref):
    pre = nn(vb, w_in_ref[0:512, :]) + nn(agg, w_in_ref[512:1024, :])
    hidden = (pre * sigmoid(pre)).astype(BF16)
    normed, inv = layer_norm(nn(hidden, w_out_ref[...]))
    return pre, hidden, normed, inv


def split_store(k, scratch_ref, keep_ref, send_ref, at, rows):
    for c in range(16):
        mine = pl.multiple_of(2 * c * rows + k * rows, 16)
        other = pl.multiple_of(2 * c * rows + (1 - k) * rows, 16)
        keep_ref[c, at : at + rows, :] = scratch_ref[pl.ds(mine, rows), :]
        send_ref[c, at : at + rows, :] = scratch_ref[pl.ds(other, rows), :]


def store_gains(edge_gain, node_gain, keep_ref, send_ref):
    pad = jnp.concatenate([edge_gain, node_gain, jnp.zeros((14, 512), F32)], axis=0).astype(BF16)
    keep_ref[16, 0:16, :] = pad
    send_ref[16, 0:16, :] = pad


def node_backward(grad, vb, agg, pre, hidden, normed, inv, w_in_ref, w_out_ref, gain, g_in_ref, g_out_ref):
    grad_gain = jnp.sum(grad * normed, axis=0, keepdims=True)
    dz = layer_norm_back(grad, gain, normed, inv).astype(BF16)
    g_out_ref[...] = tn(hidden, dz).astype(BF16)
    da = (nt(dz, w_out_ref[...]) * swish_back(pre)).astype(BF16)
    g_in_ref[0:512, :] = tn(vb, da).astype(BF16)
    g_in_ref[512:1024, :] = tn(agg, da).astype(BF16)
    return grad_gain, nt(da, w_in_ref[0:512, :]), nt(da, w_in_ref[512:1024, :])


def gather_kernel(own_ref, lists_ref, vb_ref, lists, vb, o0, o1, o2, o3, o4, sems):
    wait(Copies(sems).start((lists_ref, lists), (vb_ref.at[0], vb)))
    send_blocks(lists, own_ref[0], vb[...], (o0, o1, o2, o3, o4))


def start_weights(copies, layer, sources, targets):
    return [copies.start((source.at[layer], target)) for source, target in zip(sources, targets)]


def first_kernel(
    own_ref, slot_ref, receiver_ref, eb_ref, vb, we_in_ref, we_out_ref, wn_in_ref, wn_out_ref, e_gain_ref, n_gain_ref,
    onehot, eb, we_in, we_out, wn_in, wn_out, e_gain, n_gain, part, proj,
    slot, receiver, sems,
):
    copies = Copies(sems)
    index = copies.start((slot_ref, slot), (receiver_ref, receiver))
    loads = start_weights(copies, 0, (we_in_ref, we_out_ref, wn_in_ref, wn_out_ref), (we_in, we_out, wn_in, wn_out))
    latent = copies.start((eb_ref.at[0], eb))
    gains = copies.start((e_gain_ref, e_gain), (n_gain_ref, n_gain))
    wait(index)
    build_onehot(onehot, slot, receiver, own_ref[0])
    wait(loads[0])
    proj[0:128, :] = nn(vb[...], we_in[1024:1536, :]).astype(BF16)
    proj[128:256, :] = nn(vb[...], we_in[512:1024, :]).astype(BF16)
    wait(latent)
    part[...] = nn(eb[...], we_in[0:512, :])
    for load in loads[1:]:
        wait(load)
    wait(gains)


def second_kernel(
    state, eb, cot_ref, we_in_ref, we_out_ref, wn_in_ref, wn_out_ref,
    cot, we_in, we_out, wn_in, wn_out, part, proj, sems,
):
    copies = Copies(sems)
    loads = start_weights(copies, 1, (we_in_ref, we_out_ref, wn_in_ref, wn_out_ref), (we_in, we_out, wn_in, wn_out))
    load = copies.start((cot_ref.at[0], cot))
    vb = state[0].astype(BF16)
    wait(loads[0])
    proj[0:128, :] = nn(vb, we_in[1024:1536, :]).astype(BF16)
    proj[128:256, :] = nn(vb, we_in[512:1024, :]).astype(BF16)
    part[...] = nn(eb[...], we_in[0:512, :])
    for handles in loads[1:]:
        wait(handles)
    wait(load)


def fill_remote(proj, near, senders, vb, blocks, w_in_ref):
    senders[0:128, :] = vb
    for n, block in enumerate(blocks):
        senders[128 + 32 * n : 160 + 32 * n, :] = block[...]
    proj[0:256, :] = near[...]
    proj[256:416, :] = nn(senders[128:288, :], w_in_ref[512:1024, :]).astype(BF16)
    proj[416:512, :] = jnp.zeros((96, 512), BF16)


def forward_kernel(
    own_ref, count_ref, lists, vb_ref, onehot, eb, we_in, we_out, wn_in, wn_out, e_gain, n_gain, part, near, b0, b1, b2, b3, b4,
    state, sides, eb_next, saved_out, inv_out, o0, o1, o2, o3, o4,
    proj, message, saved, inv_s, sems,
):
    own, count = own_ref[0], count_ref[0]
    vb = vb_ref[...]
    fill_remote(proj, near, sides, vb, (b0, b1, b2, b3, b4), we_in)
    gain = e_gain[0:1, :]
    copies, saves = Copies(sems), []
    for n in range(eb.shape[0] // CHUNK):
        rows = slice(n * CHUNK, (n + 1) * CHUNK)
        pre = part[rows, :] + tn(onehot[:, rows], proj[...])
        hidden = (pre * sigmoid(pre)).astype(BF16)
        normed, inv = layer_norm(nn(hidden, we_out[...]))
        m = normed * gain * live_rows(n * CHUNK, count)
        saved[0, rows, :] = pre.astype(BF16)
        saved[1, rows, :] = normed.astype(BF16)
        inv_s[rows, :] = jnp.broadcast_to(inv, (CHUNK, 128))
        message[rows, :] = m.astype(BF16)
        eb_next[rows, :] = (eb[rows, :].astype(F32) + m).astype(BF16)
        at = pl.ds(n * CHUNK, CHUNK)
        saves += copies.start(
            (saved.at[0, at], saved_out.at[0, at]), (saved.at[1, at], saved_out.at[1, at]), (inv_s.at[at], inv_out.at[at])
        )
    agg = nn(onehot[0:128, :], message[...]).astype(BF16)
    pre, _, normed, inv = node_forward(vb, agg, wn_in, wn_out)
    v = vb.astype(F32) + normed * n_gain[0:1, :]
    state[0] = v
    state[1] = pre
    state[2] = normed
    state[3] = jnp.broadcast_to(inv, (128, 512))
    sides[288:416, :] = agg
    send_blocks(lists, own, v.astype(BF16), (o0, o1, o2, o3, o4))
    wait(saves)


def edge_tail(onehot, senders, vb, eb, h_ref, dz_ref, da_ref, we_in, g_in, g_out, outs):
    g_out[...] = tn(h_ref[...], dz_ref[...]).astype(BF16)
    g_in[0:512, :] = tn(eb[...], da_ref[...]).astype(BF16)
    gathered = nn(onehot[0:416, :], da_ref[...]).astype(BF16)
    at_receiver = gathered[0:128, :]
    at_sender = gathered[128:416, :]
    g_in[512:1024, :] = tn(senders[...], at_sender).astype(BF16)
    g_in[1024:1536, :] = tn(vb, at_receiver).astype(BF16)
    back = nt(at_sender, we_in[512:1024, :])
    for n, out in enumerate(outs):
        out[...] = back[128 + 32 * n : 160 + 32 * n, :].astype(BF16)
    return nt(at_receiver, we_in[1024:1536, :]) + back[0:128, :]


def write_grads(k, g_in, g_out, gn_in, gn_out, edge_gain, node_gain, keep, send):
    split_store(k, g_in, keep, send, 0, 48)
    split_store(k, g_out, keep, send, 48, 16)
    split_store(k, gn_in, keep, send, 64, 32)
    split_store(k, gn_out, keep, send, 96, 16)
    store_gains(edge_gain, node_gain, keep, send)


def middle_kernel(
    own_ref, count_ref, state, onehot, eb, cot, we_in, we_out, wn_in, wn_out, e_gain, n_gain, part, near, b0, b1, b2, b3, b4,
    node_out, edge_grad_out, grad_out, keep, send, o0, o1, o2, o3, o4,
    v, edge_grad, senders, proj, message, pre_s, normed_s, inv_s, hidden_s, dz_s, da_s, g_in, g_out, gn_in, gn_out, sems,
):
    own, count = own_ref[0], count_ref[0]
    vb = state[0].astype(BF16)
    fill_remote(proj, near, senders, vb, (b0, b1, b2, b3, b4), we_in)
    gain = e_gain[1:2, :]
    chunks = eb.shape[0] // CHUNK
    for n in range(chunks):
        rows = slice(n * CHUNK, (n + 1) * CHUNK)
        pre = part[rows, :] + tn(onehot[:, rows], proj[...])
        hidden = (pre * sigmoid(pre)).astype(BF16)
        normed, inv = layer_norm(nn(hidden, we_out[...]))
        m = normed * gain * live_rows(n * CHUNK, count)
        pre_s[rows, :] = pre
        normed_s[rows, :] = normed
        inv_s[rows, :] = jnp.broadcast_to(inv, (CHUNK, 128))
        hidden_s[rows, :] = hidden
        message[rows, :] = m.astype(BF16)
    agg = nn(onehot[0:128, :], message[...]).astype(BF16)
    n_pre, n_hidden, n_normed, n_inv = node_forward(vb, agg, wn_in, wn_out)
    n_gain_row = n_gain[1:2, :]
    v[...] = state[0] + n_normed * n_gain_row
    copies = Copies(sems)
    saves = copies.start((v, node_out.at[0]))
    grad = cot[...].astype(F32)
    grad_n_gain, grad_v, grad_agg = node_backward(
        grad, vb, agg, n_pre, n_hidden, n_normed, n_inv, wn_in, wn_out, n_gain_row, gn_in, gn_out
    )
    grad_agg = grad_agg.astype(BF16)
    grad_e_gain = jnp.zeros((1, 512), F32)
    for n in range(chunks):
        rows = slice(n * CHUNK, (n + 1) * CHUNK)
        gm = tn(onehot[0:128, rows], grad_agg) * live_rows(n * CHUNK, count)
        normed = normed_s[rows, :]
        grad_e_gain += jnp.sum(gm * normed, axis=0, keepdims=True)
        dz = layer_norm_back(gm, gain, normed, inv_s[rows, 0:1]).astype(BF16)
        dz_s[rows, :] = dz
        da = (nt(dz, we_out[...]) * swish_back(pre_s[rows, :])).astype(BF16)
        da_s[rows, :] = da
        edge_grad[rows, :] = nt(da, we_in[0:512, :]).astype(BF16)
        at = pl.ds(n * CHUNK, CHUNK)
        saves += copies.start((edge_grad.at[at], edge_grad_out.at[at]))
    grad_ends = edge_tail(onehot, senders, vb, eb, hidden_s, dz_s, da_s, we_in, g_in, g_out, (o0, o1, o2, o3, o4))
    grad_out[...] = grad + grad_v + grad_ends
    write_grads(own & 1, g_in, g_out, gn_in, gn_out, grad_e_gain, grad_n_gain, keep, send)
    wait(saves)


def backward_kernel(
    own_ref, count_ref, lists, onehot, grad_ref, r0, r1, r2, r3, r4, eb_ref, state_ref, sides_ref, edge_grad_ref, saved_ref, inv_ref,
    we_in_ref, we_out_ref, wn_in_ref, wn_out_ref, e_gain_ref, n_gain_ref,
    grad_out, keep, send, o0, o1, o2, o3, o4,
    eb, state, sides, edge_grad, saved, inv_s, we_in, we_out, wn_in, wn_out, e_gain, n_gain,
    hidden_s, dz_s, da_s, g_in, g_out, gn_in, gn_out, sems,
):
    own, count = own_ref[0], count_ref[0]
    copies = Copies(sems)
    node = copies.start((state_ref.at[pl.ds(1, 3)], state), (sides_ref, sides), (n_gain_ref, n_gain))
    node += copies.start((wn_out_ref.at[0], wn_out), (wn_in_ref.at[0], wn_in))
    edge = copies.start((edge_grad_ref, edge_grad), (saved_ref, saved), (inv_ref, inv_s), (e_gain_ref, e_gain), (we_out_ref.at[0], we_out))
    last = copies.start((eb_ref.at[0], eb), (we_in_ref.at[0], we_in))
    wait(node)
    vb = sides[0:128, :]
    grad = grad_ref[...] + returned(lists, own, (r0, r1, r2, r3, r4))
    n_pre = state[0]
    n_hidden = (n_pre * sigmoid(n_pre)).astype(BF16)
    grad_n_gain, grad_v, grad_agg = node_backward(
        grad, vb, sides[288:416, :], n_pre, n_hidden, state[1], state[2], wn_in, wn_out, n_gain[0:1, :], gn_in, gn_out
    )
    grad_agg = grad_agg.astype(BF16)
    wait(edge)
    gain = e_gain[0:1, :]
    grad_e_gain = jnp.zeros((1, 512), F32)
    for n in range(eb.shape[0] // CHUNK):
        rows = slice(n * CHUNK, (n + 1) * CHUNK)
        gm = tn(onehot[0:128, rows], grad_agg) + edge_grad[rows, :].astype(F32)
        gm = gm * live_rows(n * CHUNK, count)
        normed = saved[1, rows, :].astype(F32)
        grad_e_gain += jnp.sum(gm * normed, axis=0, keepdims=True)
        dz = layer_norm_back(gm, gain, normed, inv_s[rows, 0:1]).astype(BF16)
        dz_s[rows, :] = dz
        pre = saved[0, rows, :].astype(F32)
        s = sigmoid(pre)
        hidden_s[rows, :] = (pre * s).astype(BF16)
        da_s[rows, :] = (nt(dz, we_out[...]) * (s * (1.0 + pre * (1.0 - s)))).astype(BF16)
    wait(last)
    grad_ends = edge_tail(onehot, sides.at[0:288], vb, eb, hidden_s, dz_s, da_s, we_in, g_in, g_out, (o0, o1, o2, o3, o4))
    grad_out[...] = grad + grad_v + grad_ends
    write_grads(own & 1, g_in, g_out, gn_in, gn_out, grad_e_gain, grad_n_gain, keep, send)


def pack_kernel(keep_ref, recv_ref, out_ref, stage, packed, sems):
    gains = keep_ref[16, 0:16, :].astype(F32) + recv_ref[16, 0:16, :].astype(F32)
    for b in range(4):
        for q in range(4):
            stage[b, 112 + q : 113 + q, :] = gains[0:1, 128 * q : 128 * q + 128]
            stage[b, 116 + q : 117 + q, :] = gains[1:2, 128 * q : 128 * q + 128]
    copies = Copies(sems)
    saves = []
    for c in range(16):
        rows = keep_ref[c].astype(F32) + recv_ref[c].astype(F32)
        for b in range(4):
            for q in range(4):
                lanes = slice(128 * q, 128 * q + 128)
                at = 28 * q
                stage[b, at : at + 12, :] = rows[12 * b : 12 * b + 12, lanes]
                stage[b, at + 12 : at + 16, :] = rows[48 + 4 * b : 52 + 4 * b, lanes]
                stage[b, at + 16 : at + 24, :] = rows[64 + 8 * b : 72 + 8 * b, lanes]
                stage[b, at + 24 : at + 28, :] = rows[96 + 4 * b : 100 + 4 * b, lanes]
            packed[4 * c + b] = stage[b].astype(BF16)
        saves += copies.start((packed.at[pl.ds(4 * c, 4)], out_ref.at[pl.ds(4 * c, 4)]))
    wait(saves)


def sum_blocks(x):
    def step(n, total):
        return total + x[n].astype(F32)

    return lax.fori_loop(0, 64, step, jnp.zeros((120, 128), F32), unroll=8)


def pick_gains(rows, device):
    picks = lax.broadcasted_iota(jnp.int32, (128, 128), 0) - 4 * (device & 31)
    select = jnp.where(picks == lax.broadcasted_iota(jnp.int32, (128, 128), 1), 1.0, 0.0).astype(F32)
    return lax.dot_general(rows, select, (((1,), (0,)), ((), ())), precision=lax.Precision.HIGHEST, preferred_element_type=F32)


def sum_kernel(device_ref, x_ref, out_ref, gains_ref, x, sems):
    wait(Copies(sems).start((x_ref, x)))
    out_ref[...] = sum_blocks(x)
    gains_ref[...] = pick_gains(out_ref[112:120, :], device_ref[0])


def node_grad_kernel(own_ref, lists, grad_ref, r0, r1, r2, r3, r4, out_ref, total, sems):
    total[...] = grad_ref[...] + returned(lists, own_ref[0], (r0, r1, r2, r3, r4))
    wait(Copies(sems).start((total, out_ref.at[0])))


def finish_kernel(device_ref, x0_ref, total1, gains1, g_e_in, g_e_out, g_n_in, g_n_out, g_e_gain, g_n_gain, total0):
    total0[...] = sum_blocks(x0_ref)
    device = device_ref[0]
    row = lax.broadcasted_iota(jnp.int32, (8, 128), 0) - device // 32
    for layer, total in ((0, total0), (1, total1)):
        for q in range(4):
            lanes = slice(128 * q, 128 * q + 128)
            at = 28 * q
            g_e_in[:, layer, lanes] = total[at : at + 12, :]
            g_e_out[layer, :, lanes] = total[at + 12 : at + 16, :]
            g_n_in[layer, :, lanes] = total[at + 16 : at + 24, :]
            g_n_out[layer, :, lanes] = total[at + 24 : at + 28, :]
        gains = gains1[...] if layer else pick_gains(total[112:120, :], device)
        g_e_gain[layer : layer + 1, :] = jnp.sum(jnp.where(row == 0, gains, 0.0), axis=0, keepdims=True)[:, 0:4]
        g_n_gain[layer : layer + 1, :] = jnp.sum(jnp.where(row == 4, gains, 0.0), axis=0, keepdims=True)[:, 0:4]


def body(
    node_latent,
    edge_latent,
    node_cotangent,
    edge_w_in,
    edge_w_out,
    node_w_in,
    node_w_out,
    edge_gain,
    node_gain,
    edge_slot,
    edge_receiver,
    send_list,
    edge_count,
):
    width = node_latent.shape[2]
    nodes = node_latent.shape[1]
    edges = edge_slot.shape[0]
    graph = lax.axis_size("graph")
    own = lax.axis_index("graph").astype(jnp.int32)
    own_arr = own.reshape(1)
    device = (own * lax.axis_size("batch") + lax.axis_index("batch").astype(jnp.int32)).reshape(1)
    slot = edge_slot.reshape(1, edges)
    receiver = edge_receiver.reshape(1, edges)
    sds = jax.ShapeDtypeStruct
    vmem = pl.BlockSpec(memory_space=pltpu.VMEM)
    smem = pl.BlockSpec(memory_space=pltpu.SMEM)
    free = pl.BlockSpec(memory_space=pl.ANY)
    hbm = pl.BlockSpec(memory_space=pltpu.HBM)
    kept = pl.BlockSpec(memory_space=pltpu.VMEM)

    def exchange(blocks, back):
        sources = [(readers if back else neighbours)(i) for i in range(graph)]
        outs = {}
        for n in ORDER:
            outs[n] = lax.ppermute(blocks[n], "graph", [(sources[i][n], i) for i in range(graph)])
        return [outs[n] for n in range(5)]

    def call(kernel, mib, outs, scratch, specs, args):
        at = {id(hbm): pltpu.HBM, id(kept): pltpu.VMEM}
        real = {id(hbm): free, id(kept): vmem}
        shapes = [at[id(p)](o.shape, o.dtype) if id(p) in at else o for o, p in outs]
        args = [pltpu.with_memory_space_constraint(a, at[id(p)]) if id(p) in at else a for a, p in zip(args, specs)]
        return pl.pallas_call(
            kernel,
            out_shape=shapes,
            in_specs=[real.get(id(p), p) for p in specs],
            out_specs=[real.get(id(p), p) for _, p in outs],
            scratch_shapes=scratch,
            compiler_params=pltpu.CompilerParams(vmem_limit_bytes=mib * 1024 * 1024),
        )(*args)

    def vb16(*shape):
        return pltpu.VMEM(shape, BF16)

    def vf32(*shape):
        return pltpu.VMEM(shape, F32)

    def sems(n):
        return pltpu.SemaphoreType.DMA((n,))

    def ob16(*shape):
        return (sds(shape, BF16), kept)

    def of32(*shape):
        return (sds(shape, F32), kept)

    def swap(send):
        return lax.ppermute(send, "graph", [(i, i ^ 1) for i in range(graph)])

    def spread(packed):
        groups = [[(2 * c + k) * 4 + b for c in range(16) for b in range(4)] for k in range(2)]
        return lax.all_to_all(packed, ("graph", "batch"), 0, 0, tiled=True, axis_index_groups=groups)

    index_s = [pltpu.VMEM((1, edges), jnp.int32)] * 2
    weights = (edge_w_in, edge_w_out, node_w_in, node_w_out)
    weights_s = [vb16(*w.shape[1:]) for w in weights] + [vf32(*edge_gain.shape), vf32(*node_gain.shape)]
    weights_out = [ob16(*w.shape[1:]) for w in weights]
    edge_b, edge_f = vb16(edges, width), vf32(edges, width)
    grads_s = [vb16(r, width) for r in (1536, 512, 1024, 512)]
    blocks_out = [(sds((32, width), BF16), vmem)] * 5
    half = (sds((17, 112, width), BF16), vmem)

    lists, vb0, *first = call(
        gather_kernel, 2, [(sds(send_list.shape, jnp.int32), kept), ob16(nodes, width)] + blocks_out, [sems(2)],
        [smem, hbm, hbm], (own_arr, send_list, node_latent),
    )
    senders0 = exchange(first, False)
    onehot, eb0, we_in0, we_out0, wn_in0, wn_out0, e_gain, n_gain, part0, near0 = call(
        first_kernel,
        4,
        [ob16(512, edges), ob16(edges, width)] + weights_out + [of32(*edge_gain.shape), of32(*node_gain.shape), of32(edges, width), ob16(256, width)],
        index_s + [sems(12)],
        [smem, hbm, hbm, hbm, kept] + [hbm] * 6,
        (own_arr, slot, receiver, edge_latent, vb0, *weights, edge_gain, node_gain),
    )
    weights0 = (we_in0, we_out0, wn_in0, wn_out0, e_gain, n_gain)
    state, sides, eb1, saved, inv, *second = call(
        forward_kernel,
        10,
        [of32(4, nodes, width), ob16(416, width), ob16(edges, width), (sds((2, edges, width), BF16), hbm), (sds((edges, 128), F32), hbm)] + blocks_out,
        [vb16(512, width), edge_b, vb16(2, edges, width), vf32(edges, 128), sems(16)],
        [smem, smem] + [kept] * 12 + [vmem] * 5,
        (own_arr, edge_count, lists, vb0, onehot, eb0, *weights0, part0, near0, *senders0),
    )
    senders1 = exchange(second, False)
    cot, we_in1, we_out1, wn_in1, wn_out1, part1, near1 = call(
        second_kernel,
        4,
        [ob16(nodes, width)] + weights_out + [of32(edges, width), ob16(256, width)],
        [sems(8)],
        [kept, kept] + [hbm] * 5,
        (state, eb1, node_cotangent, *weights),
    )
    node_out, edge_grad, grad1, keep1, send1, *back1 = call(
        middle_kernel,
        20,
        [(sds((1, nodes, width), F32), hbm), (sds((edges, width), BF16), hbm), of32(nodes, width), half, half] + blocks_out,
        [vf32(nodes, width), edge_b, vb16(288, width), vb16(512, width), edge_b, edge_f, edge_f, vf32(edges, 128), edge_b, edge_b, edge_b] + grads_s + [sems(8)],
        [smem, smem] + [kept] * 12 + [vmem] * 5,
        (own_arr, edge_count, state, onehot, eb1, cot, we_in1, we_out1, wn_in1, wn_out1, e_gain, n_gain, part1, near1, *senders1),
    )
    packed_out = (sds((64, 120, 128), BF16), hbm)
    pack_s = [vf32(4, 120, 128), vb16(64, 120, 128), sems(16)]
    returned1 = exchange(back1, True)
    (packed1,) = call(pack_kernel, 5, [packed_out], pack_s, [vmem, vmem], (keep1, swap(send1)))
    x1 = spread(packed1)
    grad0, keep0, send0, *back0 = call(
        backward_kernel,
        22,
        [(sds((nodes, width), F32), vmem), half, half] + blocks_out,
        [edge_b, vf32(3, nodes, width), vb16(416, width), edge_b, vb16(2, edges, width), vf32(edges, 128)] + weights_s + [edge_b, edge_b, edge_b] + grads_s + [sems(12)],
        [smem, smem, kept, kept] + [vmem] * 6 + [hbm, free, free] + [hbm] * 9,
        (own_arr, edge_count, lists, onehot, grad1, *returned1, edge_latent, state, sides, edge_grad, saved, inv, *weights, edge_gain, node_gain),
    )
    returned0 = exchange(back0, True)
    (packed0,) = call(pack_kernel, 5, [packed_out], pack_s, [vmem, vmem], (keep0, swap(send0)))
    x0 = spread(packed0)
    total1, gains1 = call(
        sum_kernel, 4, [of32(120, 128), of32(8, 128)], [vb16(64, 120, 128), sems(1)], [smem, free], (device, x1)
    )
    (node_grad,) = call(
        node_grad_kernel, 2, [(sds((1, nodes, width), F32), hbm)], [vf32(nodes, width), sems(1)],
        [smem, kept, vmem] + [vmem] * 5, (own_arr, lists, grad0, *returned0),
    )
    g_e_in, *grads = call(
        finish_kernel,
        4,
        [(sds((12, 2, width), F32), vmem)] + [(sds((2, r, width), F32), vmem) for r in (4, 8, 4)] + [(sds((2, 4), F32), vmem)] * 2,
        [vf32(120, 128)],
        [smem, kept, kept, kept],
        (device, x0, total1, gains1),
    )
    return (node_out, node_grad, jnp.swapaxes(g_e_in, 0, 1), *grads)


def solution(mesh):
    in_specs = (
        P("batch", "graph", None),
        P("batch", "graph", None),
        P("batch", "graph", None),
        P(),
        P(),
        P(),
        P(),
        P(),
        P(),
        P("graph"),
        P("graph"),
        P("graph", None),
        P("graph"),
    )
    out_specs = (
        P("batch", "graph", None),
        P("batch", "graph", None),
        P(None, ("graph", "batch"), None),
        P(None, ("graph", "batch"), None),
        P(None, ("graph", "batch"), None),
        P(None, ("graph", "batch"), None),
        P(None, ("graph", "batch")),
        P(None, ("graph", "batch")),
    )
    return jax.shard_map(body, mesh=mesh, in_specs=in_specs, out_specs=out_specs, check_vma=False)
```

```python
import jax
import jax.numpy as jnp
from jax import lax
from jax.experimental import pallas as pl
from jax.experimental.pallas import tpu as pltpu
from jax.sharding import PartitionSpec as P


EPSILON = 1e-05
CHUNK = 512
ORDER = (4, 2, 3, 1, 0)
F32 = jnp.float32
BF16 = jnp.bfloat16


def nn(a, b):
    return lax.dot_general(a, b, (((1,), (0,)), ((), ())), preferred_element_type=F32)


def nt(a, b):
    return lax.dot_general(a, b, (((1,), (1,)), ((), ())), preferred_element_type=F32)


def tn(a, b):
    return lax.dot_general(a, b, (((0,), (0,)), ((), ())), preferred_element_type=F32)


def sigmoid(x):
    return 0.5 * jnp.tanh(0.5 * x) + 0.5


def layer_norm(z):
    centre = z - jnp.mean(z, axis=-1, keepdims=True)
    inv = lax.rsqrt(jnp.mean(centre * centre, axis=-1, keepdims=True) + EPSILON)
    return centre * inv, inv


def layer_norm_back(grad, gain, normed, inv):
    gn = grad * gain
    m1 = jnp.mean(gn, axis=-1, keepdims=True)
    m2 = jnp.mean(gn * normed, axis=-1, keepdims=True)
    return inv * (gn - m1 - normed * m2)


def swish_back(pre):
    s = sigmoid(pre)
    return s * (1.0 + pre * (1.0 - s))


def near(own):
    return ((((own - 1) & 31) ^ 1) + 1) & 31


def neighbours(own):
    return own ^ 1, near(own), near(own) ^ 1, near(own ^ 1), own ^ 16


def readers(own):
    return own ^ 1, near(own), near(own ^ 1), near(own) ^ 1, own ^ 16


def list_onehot(lists_ref, reader, nodes):
    row = lists_ref[pl.ds(reader, 1), :]
    ids = lax.broadcasted_iota(jnp.int32, (nodes, row.shape[1]), 0)
    return jnp.where(ids == row, 1.0, 0.0).astype(BF16)


def send_blocks(lists_ref, own, vb, outs):
    swap, pair, side, far = outs
    for reader, (out, at) in zip(readers(own), ((swap, 0), (pair, 0), (side, 0), (pair, 32), (far, 0))):
        onehot = list_onehot(lists_ref, reader, vb.shape[0])
        out[at : at + 32, :] = tn(onehot, vb).astype(BF16)


def returned(lists_ref, own, blocks):
    total = None
    for reader, block in zip(readers(own), blocks):
        term = nn(list_onehot(lists_ref, reader, 128), block[...])
        total = term if total is None else total + term
    return total


class Copies:
    def __init__(self, sems):
        self.sems, self.count = sems, 0

    def start(self, *pairs):
        handles = []
        for source, target in pairs:
            handles.append(pltpu.make_async_copy(source, target, self.sems.at[self.count]))
            self.count += 1
        for handle in handles:
            handle.start()
        return handles


def wait(handles):
    for handle in handles:
        handle.wait()


def build_onehot(onehot_ref, slot_ref, receiver_ref, own):
    edges = slot_ref.shape[1]
    slot = slot_ref[...]
    row = slot - 128
    source = row >> 5
    block = jnp.full(source.shape, 4, jnp.int32)
    for n, other in enumerate(neighbours(own)[:4]):
        block = jnp.where(source == other, n, block)
    position = jnp.where(slot < 128, slot, 128 + block * 32 + (row & 31))
    ids = lax.broadcasted_iota(jnp.int32, (128, edges), 0)
    onehot_ref[0:128, :] = jnp.where(ids == receiver_ref[...], 1.0, 0.0).astype(BF16)
    ids = lax.broadcasted_iota(jnp.int32, (384, edges), 0)
    onehot_ref[128:512, :] = jnp.where(ids == position, 1.0, 0.0).astype(BF16)


def live_rows(base, count):
    rows = base + lax.broadcasted_iota(jnp.int32, (CHUNK, 1), 0)
    return jnp.where(rows < count, 1.0, 0.0).astype(F32)


def node_forward(vb, agg, w_in_ref, w_out_ref):
    pre = nn(vb, w_in_ref[0:512, :]) + nn(agg, w_in_ref[512:1024, :])
    hidden = (pre * sigmoid(pre)).astype(BF16)
    normed, inv = layer_norm(nn(hidden, w_out_ref[...]))
    return pre, hidden, normed, inv


def split_store(k, scratch_ref, keep_ref, send_ref, at, rows):
    for c in range(16):
        mine = pl.multiple_of(2 * c * rows + k * rows, 16)
        other = pl.multiple_of(2 * c * rows + (1 - k) * rows, 16)
        keep_ref[c, at : at + rows, :] = scratch_ref[pl.ds(mine, rows), :]
        send_ref[c, at : at + rows, :] = scratch_ref[pl.ds(other, rows), :]


def store_gains(edge_gain, node_gain, keep_ref, send_ref):
    pad = jnp.concatenate([edge_gain, node_gain, jnp.zeros((14, 512), F32)], axis=0).astype(BF16)
    keep_ref[16, 0:16, :] = pad
    send_ref[16, 0:16, :] = pad


def node_backward(grad, vb, agg, pre, hidden, normed, inv, w_in_ref, w_out_ref, gain, g_in_ref, g_out_ref):
    grad_gain = jnp.sum(grad * normed, axis=0, keepdims=True)
    dz = layer_norm_back(grad, gain, normed, inv).astype(BF16)
    g_out_ref[...] = tn(hidden, dz).astype(BF16)
    da = (nt(dz, w_out_ref[...]) * swish_back(pre)).astype(BF16)
    g_in_ref[0:512, :] = tn(vb, da).astype(BF16)
    g_in_ref[512:1024, :] = tn(agg, da).astype(BF16)
    return grad_gain, nt(da, w_in_ref[0:512, :]), nt(da, w_in_ref[512:1024, :])


def gather_kernel(own_ref, lists_ref, vb_ref, lists, vb, o0, o1, o2, o3, sems):
    wait(Copies(sems).start((lists_ref, lists), (vb_ref.at[0], vb)))
    send_blocks(lists, own_ref[0], vb[...], (o0, o1, o2, o3))


def start_weights(copies, layer, sources, targets):
    return [copies.start((source.at[layer], target)) for source, target in zip(sources, targets)]


def first_kernel(
    own_ref, slot_ref, receiver_ref, eb_ref, vb, we_in_ref, we_out_ref, wn_in_ref, wn_out_ref, e_gain_ref, n_gain_ref,
    onehot, eb, we_in, we_out, wn_in, wn_out, e_gain, n_gain, part, proj,
    slot, receiver, sems,
):
    copies = Copies(sems)
    index = copies.start((slot_ref, slot), (receiver_ref, receiver))
    loads = start_weights(copies, 0, (we_in_ref, we_out_ref, wn_in_ref, wn_out_ref), (we_in, we_out, wn_in, wn_out))
    latent = copies.start((eb_ref.at[0], eb))
    gains = copies.start((e_gain_ref, e_gain), (n_gain_ref, n_gain))
    wait(index)
    build_onehot(onehot, slot, receiver, own_ref[0])
    wait(loads[0])
    proj[0:128, :] = nn(vb[...], we_in[1024:1536, :]).astype(BF16)
    proj[128:256, :] = nn(vb[...], we_in[512:1024, :]).astype(BF16)
    wait(latent)
    part[...] = nn(eb[...], we_in[0:512, :])
    for load in loads[1:]:
        wait(load)
    wait(gains)


def second_kernel(
    state, eb, cot_ref, we_in_ref, we_out_ref, wn_in_ref, wn_out_ref,
    cot, we_in, we_out, wn_in, wn_out, part, proj, sems,
):
    copies = Copies(sems)
    loads = start_weights(copies, 1, (we_in_ref, we_out_ref, wn_in_ref, wn_out_ref), (we_in, we_out, wn_in, wn_out))
    load = copies.start((cot_ref.at[0], cot))
    vb = state[0].astype(BF16)
    wait(loads[0])
    proj[0:128, :] = nn(vb, we_in[1024:1536, :]).astype(BF16)
    proj[128:256, :] = nn(vb, we_in[512:1024, :]).astype(BF16)
    part[...] = nn(eb[...], we_in[0:512, :])
    for handles in loads[1:]:
        wait(handles)
    wait(load)


def fill_remote(proj, near, senders, vb, blocks, w_in_ref):
    senders[0:128, :] = vb
    for n, (block, at) in enumerate(zip(blocks, (0, 0, 0, 32, 0))):
        senders[128 + 32 * n : 160 + 32 * n, :] = block[at : at + 32, :]
    proj[0:256, :] = near[...]
    proj[256:416, :] = nn(senders[128:288, :], w_in_ref[512:1024, :]).astype(BF16)
    proj[416:512, :] = jnp.zeros((96, 512), BF16)


def forward_kernel(
    own_ref, count_ref, lists, vb_ref, onehot, eb, we_in, we_out, wn_in, wn_out, e_gain, n_gain, part, near, b0, b1, b2, b3, b4,
    state, sides, eb_next, saved_out, inv_out, o0, o1, o2, o3,
    proj, message, saved, inv_s, sems,
):
    own, count = own_ref[0], count_ref[0]
    vb = vb_ref[...]
    fill_remote(proj, near, sides, vb, (b0, b1, b2, b3, b4), we_in)
    gain = e_gain[0:1, :]
    copies, saves = Copies(sems), []
    for n in range(eb.shape[0] // CHUNK):
        rows = slice(n * CHUNK, (n + 1) * CHUNK)
        pre = part[rows, :] + tn(onehot[:, rows], proj[...])
        hidden = (pre * sigmoid(pre)).astype(BF16)
        normed, inv = layer_norm(nn(hidden, we_out[...]))
        m = normed * gain * live_rows(n * CHUNK, count)
        saved[0, rows, :] = pre.astype(BF16)
        saved[1, rows, :] = normed.astype(BF16)
        inv_s[rows, :] = jnp.broadcast_to(inv, (CHUNK, 128))
        message[rows, :] = m.astype(BF16)
        eb_next[rows, :] = (eb[rows, :].astype(F32) + m).astype(BF16)
        at = pl.ds(n * CHUNK, CHUNK)
        saves += copies.start(
            (saved.at[0, at], saved_out.at[0, at]), (saved.at[1, at], saved_out.at[1, at]), (inv_s.at[at], inv_out.at[at])
        )
    agg = nn(onehot[0:128, :], message[...]).astype(BF16)
    pre, _, normed, inv = node_forward(vb, agg, wn_in, wn_out)
    v = vb.astype(F32) + normed * n_gain[0:1, :]
    state[0] = v
    state[1] = pre
    state[2] = normed
    state[3] = jnp.broadcast_to(inv, (128, 512))
    sides[288:416, :] = agg
    send_blocks(lists, own, v.astype(BF16), (o0, o1, o2, o3))
    wait(saves)


def edge_tail(onehot, senders, vb, eb, h_ref, dz_ref, da_ref, we_in, g_in, g_out, outs):
    g_out[...] = tn(h_ref[...], dz_ref[...]).astype(BF16)
    g_in[0:512, :] = tn(eb[...], da_ref[...]).astype(BF16)
    gathered = nn(onehot[0:416, :], da_ref[...]).astype(BF16)
    at_receiver = gathered[0:128, :]
    at_sender = gathered[128:416, :]
    g_in[512:1024, :] = tn(senders[...], at_sender).astype(BF16)
    g_in[1024:1536, :] = tn(vb, at_receiver).astype(BF16)
    back = nt(at_sender, we_in[512:1024, :])
    for n, out in enumerate(outs):
        out[...] = back[128 + 32 * n : 160 + 32 * n, :].astype(BF16)
    return nt(at_receiver, we_in[1024:1536, :]) + back[0:128, :]


def write_grads(k, g_in, g_out, gn_in, gn_out, edge_gain, node_gain, keep, send):
    split_store(k, g_in, keep, send, 0, 48)
    split_store(k, g_out, keep, send, 48, 16)
    split_store(k, gn_in, keep, send, 64, 32)
    split_store(k, gn_out, keep, send, 96, 16)
    store_gains(edge_gain, node_gain, keep, send)


def middle_kernel(
    own_ref, count_ref, state, onehot, eb, cot, we_in, we_out, wn_in, wn_out, e_gain, n_gain, part, near, b0, b1, b2, b3, b4,
    node_out, edge_grad_out, grad_out, keep, send, o0, o1, o2, o3, o4,
    v, edge_grad, senders, proj, message, pre_s, normed_s, inv_s, hidden_s, dz_s, da_s, g_in, g_out, gn_in, gn_out, sems,
):
    own, count = own_ref[0], count_ref[0]
    vb = state[0].astype(BF16)
    fill_remote(proj, near, senders, vb, (b0, b1, b2, b3, b4), we_in)
    gain = e_gain[1:2, :]
    chunks = eb.shape[0] // CHUNK
    for n in range(chunks):
        rows = slice(n * CHUNK, (n + 1) * CHUNK)
        pre = part[rows, :] + tn(onehot[:, rows], proj[...])
        hidden = (pre * sigmoid(pre)).astype(BF16)
        normed, inv = layer_norm(nn(hidden, we_out[...]))
        m = normed * gain * live_rows(n * CHUNK, count)
        pre_s[rows, :] = pre
        normed_s[rows, :] = normed
        inv_s[rows, :] = jnp.broadcast_to(inv, (CHUNK, 128))
        hidden_s[rows, :] = hidden
        message[rows, :] = m.astype(BF16)
    agg = nn(onehot[0:128, :], message[...]).astype(BF16)
    n_pre, n_hidden, n_normed, n_inv = node_forward(vb, agg, wn_in, wn_out)
    n_gain_row = n_gain[1:2, :]
    v[...] = state[0] + n_normed * n_gain_row
    copies = Copies(sems)
    saves = copies.start((v, node_out.at[0]))
    grad = cot[...].astype(F32)
    grad_n_gain, grad_v, grad_agg = node_backward(
        grad, vb, agg, n_pre, n_hidden, n_normed, n_inv, wn_in, wn_out, n_gain_row, gn_in, gn_out
    )
    grad_agg = grad_agg.astype(BF16)
    grad_e_gain = jnp.zeros((1, 512), F32)
    for n in range(chunks):
        rows = slice(n * CHUNK, (n + 1) * CHUNK)
        gm = tn(onehot[0:128, rows], grad_agg) * live_rows(n * CHUNK, count)
        normed = normed_s[rows, :]
        grad_e_gain += jnp.sum(gm * normed, axis=0, keepdims=True)
        dz = layer_norm_back(gm, gain, normed, inv_s[rows, 0:1]).astype(BF16)
        dz_s[rows, :] = dz
        da = (nt(dz, we_out[...]) * swish_back(pre_s[rows, :])).astype(BF16)
        da_s[rows, :] = da
        edge_grad[rows, :] = nt(da, we_in[0:512, :]).astype(BF16)
        at = pl.ds(n * CHUNK, CHUNK)
        saves += copies.start((edge_grad.at[at], edge_grad_out.at[at]))
    grad_ends = edge_tail(onehot, senders, vb, eb, hidden_s, dz_s, da_s, we_in, g_in, g_out, (o0, o1, o2, o3, o4))
    grad_out[...] = grad + grad_v + grad_ends
    write_grads(own & 1, g_in, g_out, gn_in, gn_out, grad_e_gain, grad_n_gain, keep, send)
    wait(saves)


def backward_kernel(
    own_ref, count_ref, lists, onehot, grad_ref, r0, r1, r2, r3, r4, eb_ref, state_ref, sides_ref, edge_grad_ref, saved_ref, inv_ref,
    we_in_ref, we_out_ref, wn_in_ref, wn_out_ref, e_gain_ref, n_gain_ref,
    grad_out, keep, send, o0, o1, o2, o3, o4,
    eb, state, sides, edge_grad, saved, inv_s, we_in, we_out, wn_in, wn_out, e_gain, n_gain,
    hidden_s, dz_s, da_s, g_in, g_out, gn_in, gn_out, sems,
):
    own, count = own_ref[0], count_ref[0]
    copies = Copies(sems)
    node = copies.start((state_ref.at[pl.ds(1, 3)], state), (sides_ref, sides), (n_gain_ref, n_gain))
    node += copies.start((wn_out_ref.at[0], wn_out), (wn_in_ref.at[0], wn_in))
    edge = copies.start((edge_grad_ref, edge_grad), (saved_ref, saved), (inv_ref, inv_s), (e_gain_ref, e_gain), (we_out_ref.at[0], we_out))
    last = copies.start((eb_ref.at[0], eb), (we_in_ref.at[0], we_in))
    wait(node)
    vb = sides[0:128, :]
    grad = grad_ref[...] + returned(lists, own, (r0, r1, r2, r3, r4))
    n_pre = state[0]
    n_hidden = (n_pre * sigmoid(n_pre)).astype(BF16)
    grad_n_gain, grad_v, grad_agg = node_backward(
        grad, vb, sides[288:416, :], n_pre, n_hidden, state[1], state[2], wn_in, wn_out, n_gain[0:1, :], gn_in, gn_out
    )
    grad_agg = grad_agg.astype(BF16)
    wait(edge)
    gain = e_gain[0:1, :]
    grad_e_gain = jnp.zeros((1, 512), F32)
    for n in range(eb.shape[0] // CHUNK):
        rows = slice(n * CHUNK, (n + 1) * CHUNK)
        gm = tn(onehot[0:128, rows], grad_agg) + edge_grad[rows, :].astype(F32)
        gm = gm * live_rows(n * CHUNK, count)
        normed = saved[1, rows, :].astype(F32)
        grad_e_gain += jnp.sum(gm * normed, axis=0, keepdims=True)
        dz = layer_norm_back(gm, gain, normed, inv_s[rows, 0:1]).astype(BF16)
        dz_s[rows, :] = dz
        pre = saved[0, rows, :].astype(F32)
        s = sigmoid(pre)
        hidden_s[rows, :] = (pre * s).astype(BF16)
        da_s[rows, :] = (nt(dz, we_out[...]) * (s * (1.0 + pre * (1.0 - s)))).astype(BF16)
    wait(last)
    grad_ends = edge_tail(onehot, sides.at[0:288], vb, eb, hidden_s, dz_s, da_s, we_in, g_in, g_out, (o0, o1, o2, o3, o4))
    grad_out[...] = grad + grad_v + grad_ends
    write_grads(own & 1, g_in, g_out, gn_in, gn_out, grad_e_gain, grad_n_gain, keep, send)


def pack_kernel(keep_ref, recv_ref, out_ref, stage, packed, sems):
    gains = keep_ref[16, 0:16, :].astype(F32) + recv_ref[16, 0:16, :].astype(F32)
    for b in range(4):
        for q in range(4):
            stage[b, 112 + q : 113 + q, :] = gains[0:1, 128 * q : 128 * q + 128]
            stage[b, 116 + q : 117 + q, :] = gains[1:2, 128 * q : 128 * q + 128]
    copies = Copies(sems)
    saves = []
    for c in range(16):
        rows = keep_ref[c].astype(F32) + recv_ref[c].astype(F32)
        for b in range(4):
            for q in range(4):
                lanes = slice(128 * q, 128 * q + 128)
                at = 28 * q
                stage[b, at : at + 12, :] = rows[12 * b : 12 * b + 12, lanes]
                stage[b, at + 12 : at + 16, :] = rows[48 + 4 * b : 52 + 4 * b, lanes]
                stage[b, at + 16 : at + 24, :] = rows[64 + 8 * b : 72 + 8 * b, lanes]
                stage[b, at + 24 : at + 28, :] = rows[96 + 4 * b : 100 + 4 * b, lanes]
            packed[4 * c + b] = stage[b].astype(BF16)
        saves += copies.start((packed.at[pl.ds(4 * c, 4)], out_ref.at[pl.ds(4 * c, 4)]))
    wait(saves)


def sum_blocks(x):
    def step(n, total):
        return total + x[n].astype(F32)

    return lax.fori_loop(0, 64, step, jnp.zeros((120, 128), F32), unroll=8)


def pick_gains(rows, device):
    picks = lax.broadcasted_iota(jnp.int32, (128, 128), 0) - 4 * (device & 31)
    select = jnp.where(picks == lax.broadcasted_iota(jnp.int32, (128, 128), 1), 1.0, 0.0).astype(F32)
    return lax.dot_general(rows, select, (((1,), (0,)), ((), ())), precision=lax.Precision.HIGHEST, preferred_element_type=F32)


def sum_kernel(device_ref, x_ref, out_ref, gains_ref, x, sems):
    wait(Copies(sems).start((x_ref, x)))
    out_ref[...] = sum_blocks(x)
    gains_ref[...] = pick_gains(out_ref[112:120, :], device_ref[0])


def node_grad_kernel(own_ref, lists, grad_ref, r0, r1, r2, r3, r4, out_ref, total, sems):
    total[...] = grad_ref[...] + returned(lists, own_ref[0], (r0, r1, r2, r3, r4))
    wait(Copies(sems).start((total, out_ref.at[0])))


def finish_kernel(device_ref, x0_ref, total1, gains1, g_e_in, g_e_out, g_n_in, g_n_out, g_e_gain, g_n_gain, total0):
    total0[...] = sum_blocks(x0_ref)
    device = device_ref[0]
    row = lax.broadcasted_iota(jnp.int32, (8, 128), 0) - device // 32
    for layer, total in ((0, total0), (1, total1)):
        for q in range(4):
            lanes = slice(128 * q, 128 * q + 128)
            at = 28 * q
            g_e_in[:, layer, lanes] = total[at : at + 12, :]
            g_e_out[layer, :, lanes] = total[at + 12 : at + 16, :]
            g_n_in[layer, :, lanes] = total[at + 16 : at + 24, :]
            g_n_out[layer, :, lanes] = total[at + 24 : at + 28, :]
        gains = gains1[...] if layer else pick_gains(total[112:120, :], device)
        g_e_gain[layer : layer + 1, :] = jnp.sum(jnp.where(row == 0, gains, 0.0), axis=0, keepdims=True)[:, 0:4]
        g_n_gain[layer : layer + 1, :] = jnp.sum(jnp.where(row == 4, gains, 0.0), axis=0, keepdims=True)[:, 0:4]


def body(
    node_latent,
    edge_latent,
    node_cotangent,
    edge_w_in,
    edge_w_out,
    node_w_in,
    node_w_out,
    edge_gain,
    node_gain,
    edge_slot,
    edge_receiver,
    send_list,
    edge_count,
):
    width = node_latent.shape[2]
    nodes = node_latent.shape[1]
    edges = edge_slot.shape[0]
    graph = lax.axis_size("graph")
    own = lax.axis_index("graph").astype(jnp.int32)
    own_arr = own.reshape(1)
    device = (own * lax.axis_size("batch") + lax.axis_index("batch").astype(jnp.int32)).reshape(1)
    slot = edge_slot.reshape(1, edges)
    receiver = edge_receiver.reshape(1, edges)
    sds = jax.ShapeDtypeStruct
    vmem = pl.BlockSpec(memory_space=pltpu.VMEM)
    smem = pl.BlockSpec(memory_space=pltpu.SMEM)
    free = pl.BlockSpec(memory_space=pl.ANY)
    hbm = pl.BlockSpec(memory_space=pltpu.HBM)
    kept = pl.BlockSpec(memory_space=pltpu.VMEM)

    def move(block, source):
        return lax.ppermute(block, "graph", [(source(i), i) for i in range(graph)])

    def fetch(blocks):
        swap, pair, side, far = blocks
        pair = move(pair, near)
        side, far, swap = move(side, lambda i: near(i) ^ 1), move(far, lambda i: i ^ 16), move(swap, lambda i: i ^ 1)
        return swap, pair, side, move(pair, lambda i: i ^ 1), far

    def give_back(blocks):
        outs = {}
        for n in ORDER:
            outs[n] = move(blocks[n], lambda i, n=n: readers(i)[n])
        return [outs[n] for n in range(5)]

    def call(kernel, mib, outs, scratch, specs, args):
        at = {id(hbm): pltpu.HBM, id(kept): pltpu.VMEM}
        real = {id(hbm): free, id(kept): vmem}
        shapes = [at[id(p)](o.shape, o.dtype) if id(p) in at else o for o, p in outs]
        args = [pltpu.with_memory_space_constraint(a, at[id(p)]) if id(p) in at else a for a, p in zip(args, specs)]
        return pl.pallas_call(
            kernel,
            out_shape=shapes,
            in_specs=[real.get(id(p), p) for p in specs],
            out_specs=[real.get(id(p), p) for _, p in outs],
            scratch_shapes=scratch,
            compiler_params=pltpu.CompilerParams(vmem_limit_bytes=mib * 1024 * 1024),
        )(*args)

    def vb16(*shape):
        return pltpu.VMEM(shape, BF16)

    def vf32(*shape):
        return pltpu.VMEM(shape, F32)

    def sems(n):
        return pltpu.SemaphoreType.DMA((n,))

    def ob16(*shape):
        return (sds(shape, BF16), kept)

    def of32(*shape):
        return (sds(shape, F32), kept)

    def swap(send):
        return lax.ppermute(send, "graph", [(i, i ^ 1) for i in range(graph)])

    def spread(packed):
        groups = [[(2 * c + k) * 4 + b for c in range(16) for b in range(4)] for k in range(2)]
        return lax.all_to_all(packed, ("graph", "batch"), 0, 0, tiled=True, axis_index_groups=groups)

    index_s = [pltpu.VMEM((1, edges), jnp.int32)] * 2
    weights = (edge_w_in, edge_w_out, node_w_in, node_w_out)
    weights_s = [vb16(*w.shape[1:]) for w in weights] + [vf32(*edge_gain.shape), vf32(*node_gain.shape)]
    weights_out = [ob16(*w.shape[1:]) for w in weights]
    edge_b, edge_f = vb16(edges, width), vf32(edges, width)
    grads_s = [vb16(r, width) for r in (1536, 512, 1024, 512)]
    blocks_out = [(sds((32, width), BF16), vmem)] * 5
    fetch_out = [(sds((r, width), BF16), vmem) for r in (32, 64, 32, 32)]
    half = (sds((17, 112, width), BF16), vmem)

    lists, vb0, *first = call(
        gather_kernel, 2, [(sds(send_list.shape, jnp.int32), kept), ob16(nodes, width)] + fetch_out, [sems(2)],
        [smem, hbm, hbm], (own_arr, send_list, node_latent),
    )
    senders0 = fetch(first)
    onehot, eb0, we_in0, we_out0, wn_in0, wn_out0, e_gain, n_gain, part0, near0 = call(
        first_kernel,
        4,
        [ob16(512, edges), ob16(edges, width)] + weights_out + [of32(*edge_gain.shape), of32(*node_gain.shape), of32(edges, width), ob16(256, width)],
        index_s + [sems(12)],
        [smem, hbm, hbm, hbm, kept] + [hbm] * 6,
        (own_arr, slot, receiver, edge_latent, vb0, *weights, edge_gain, node_gain),
    )
    weights0 = (we_in0, we_out0, wn_in0, wn_out0, e_gain, n_gain)
    state, sides, eb1, saved, inv, *second = call(
        forward_kernel,
        10,
        [of32(4, nodes, width), ob16(416, width), ob16(edges, width), (sds((2, edges, width), BF16), hbm), (sds((edges, 128), F32), hbm)] + fetch_out,
        [vb16(512, width), edge_b, vb16(2, edges, width), vf32(edges, 128), sems(16)],
        [smem, smem] + [kept] * 12 + [vmem] * 5,
        (own_arr, edge_count, lists, vb0, onehot, eb0, *weights0, part0, near0, *senders0),
    )
    senders1 = fetch(second)
    cot, we_in1, we_out1, wn_in1, wn_out1, part1, near1 = call(
        second_kernel,
        4,
        [ob16(nodes, width)] + weights_out + [of32(edges, width), ob16(256, width)],
        [sems(8)],
        [kept, kept] + [hbm] * 5,
        (state, eb1, node_cotangent, *weights),
    )
    node_out, edge_grad, grad1, keep1, send1, *back1 = call(
        middle_kernel,
        20,
        [(sds((1, nodes, width), F32), hbm), (sds((edges, width), BF16), hbm), of32(nodes, width), half, half] + blocks_out,
        [vf32(nodes, width), edge_b, vb16(288, width), vb16(512, width), edge_b, edge_f, edge_f, vf32(edges, 128), edge_b, edge_b, edge_b] + grads_s + [sems(8)],
        [smem, smem] + [kept] * 12 + [vmem] * 5,
        (own_arr, edge_count, state, onehot, eb1, cot, we_in1, we_out1, wn_in1, wn_out1, e_gain, n_gain, part1, near1, *senders1),
    )
    packed_out = (sds((64, 120, 128), BF16), hbm)
    pack_s = [vf32(4, 120, 128), vb16(64, 120, 128), sems(16)]
    returned1 = give_back(back1)
    (packed1,) = call(pack_kernel, 5, [packed_out], pack_s, [vmem, vmem], (keep1, swap(send1)))
    x1 = spread(packed1)
    grad0, keep0, send0, *back0 = call(
        backward_kernel,
        22,
        [(sds((nodes, width), F32), vmem), half, half] + blocks_out,
        [edge_b, vf32(3, nodes, width), vb16(416, width), edge_b, vb16(2, edges, width), vf32(edges, 128)] + weights_s + [edge_b, edge_b, edge_b] + grads_s + [sems(12)],
        [smem, smem, kept, kept] + [vmem] * 6 + [hbm, free, free] + [hbm] * 9,
        (own_arr, edge_count, lists, onehot, grad1, *returned1, edge_latent, state, sides, edge_grad, saved, inv, *weights, edge_gain, node_gain),
    )
    returned0 = give_back(back0)
    (packed0,) = call(pack_kernel, 5, [packed_out], pack_s, [vmem, vmem], (keep0, swap(send0)))
    x0 = spread(packed0)
    total1, gains1 = call(
        sum_kernel, 4, [of32(120, 128), of32(8, 128)], [vb16(64, 120, 128), sems(1)], [smem, free], (device, x1)
    )
    (node_grad,) = call(
        node_grad_kernel, 2, [(sds((1, nodes, width), F32), hbm)], [vf32(nodes, width), sems(1)],
        [smem, kept, vmem] + [vmem] * 5, (own_arr, lists, grad0, *returned0),
    )
    g_e_in, *grads = call(
        finish_kernel,
        4,
        [(sds((12, 2, width), F32), vmem)] + [(sds((2, r, width), F32), vmem) for r in (4, 8, 4)] + [(sds((2, 4), F32), vmem)] * 2,
        [vf32(120, 128)],
        [smem, kept, kept, kept],
        (device, x0, total1, gains1),
    )
    return (node_out, node_grad, jnp.swapaxes(g_e_in, 0, 1), *grads)


def solution(mesh):
    in_specs = (
        P("batch", "graph", None),
        P("batch", "graph", None),
        P("batch", "graph", None),
        P(),
        P(),
        P(),
        P(),
        P(),
        P(),
        P("graph"),
        P("graph"),
        P("graph", None),
        P("graph"),
    )
    out_specs = (
        P("batch", "graph", None),
        P("batch", "graph", None),
        P(None, ("graph", "batch"), None),
        P(None, ("graph", "batch"), None),
        P(None, ("graph", "batch"), None),
        P(None, ("graph", "batch"), None),
        P(None, ("graph", "batch")),
        P(None, ("graph", "batch")),
    )
    return jax.shard_map(body, mesh=mesh, in_specs=in_specs, out_specs=out_specs, check_vma=False)
```

```python
import jax
import jax.numpy as jnp
from jax import lax
from jax.experimental import pallas as pl
from jax.experimental.pallas import tpu as pltpu
from jax.sharding import PartitionSpec as P


EPSILON = 1e-05
CHUNK = 512
F32 = jnp.float32
BF16 = jnp.bfloat16


def nn(a, b):
    return lax.dot_general(a, b, (((1,), (0,)), ((), ())), preferred_element_type=F32)


def nt(a, b):
    return lax.dot_general(a, b, (((1,), (1,)), ((), ())), preferred_element_type=F32)


def tn(a, b):
    return lax.dot_general(a, b, (((0,), (0,)), ((), ())), preferred_element_type=F32)


def sigmoid(x):
    return 0.5 * jnp.tanh(0.5 * x) + 0.5


def layer_norm(z):
    centre = z - jnp.mean(z, axis=-1, keepdims=True)
    inv = lax.rsqrt(jnp.mean(centre * centre, axis=-1, keepdims=True) + EPSILON)
    return centre * inv, inv


def layer_norm_back(grad, gain, normed, inv):
    gn = grad * gain
    m1 = jnp.mean(gn, axis=-1, keepdims=True)
    m2 = jnp.mean(gn * normed, axis=-1, keepdims=True)
    return inv * (gn - m1 - normed * m2)


def swish_back(pre):
    s = sigmoid(pre)
    return s * (1.0 + pre * (1.0 - s))


def near(own):
    return ((((own - 1) & 31) ^ 1) + 1) & 31


def neighbours(own):
    return own ^ 1, near(own), near(own) ^ 1, near(own ^ 1), own ^ 16


def readers(own):
    return own ^ 1, near(own), near(own ^ 1), near(own) ^ 1, own ^ 16


def list_onehot(lists_ref, reader, nodes):
    row = lists_ref[pl.ds(reader, 1), :]
    ids = lax.broadcasted_iota(jnp.int32, (nodes, row.shape[1]), 0)
    return jnp.where(ids == row, 1.0, 0.0).astype(BF16)


def send_blocks(lists_ref, own, vb, outs):
    swap, pair, side, far = outs
    for reader, (out, at) in zip(readers(own), ((swap, 0), (pair, 0), (side, 0), (pair, 32), (far, 0))):
        onehot = list_onehot(lists_ref, reader, vb.shape[0])
        out[at : at + 32, :] = tn(onehot, vb).astype(BF16)


def returned(lists_ref, own, blocks):
    swap, pair, side, far = blocks
    total = None
    for reader, (block, at) in zip(readers(own), ((swap, 0), (pair, 0), (side, 0), (pair, 32), (far, 0))):
        term = nn(list_onehot(lists_ref, reader, 128), block[at : at + 32, :])
        total = term if total is None else total + term
    return total


class Copies:
    def __init__(self, sems):
        self.sems, self.count = sems, 0

    def start(self, *pairs):
        handles = []
        for source, target in pairs:
            handles.append(pltpu.make_async_copy(source, target, self.sems.at[self.count]))
            self.count += 1
        for handle in handles:
            handle.start()
        return handles


def wait(handles):
    for handle in handles:
        handle.wait()


def build_onehot(onehot_ref, slot_ref, receiver_ref, own):
    edges = slot_ref.shape[1]
    slot = slot_ref[...]
    row = slot - 128
    source = row >> 5
    block = jnp.full(source.shape, 4, jnp.int32)
    for n, other in enumerate(neighbours(own)[:4]):
        block = jnp.where(source == other, n, block)
    position = jnp.where(slot < 128, slot, 128 + block * 32 + (row & 31))
    ids = lax.broadcasted_iota(jnp.int32, (128, edges), 0)
    onehot_ref[0:128, :] = jnp.where(ids == receiver_ref[...], 1.0, 0.0).astype(BF16)
    ids = lax.broadcasted_iota(jnp.int32, (384, edges), 0)
    onehot_ref[128:512, :] = jnp.where(ids == position, 1.0, 0.0).astype(BF16)


def live_rows(base, count):
    rows = base + lax.broadcasted_iota(jnp.int32, (CHUNK, 1), 0)
    return jnp.where(rows < count, 1.0, 0.0).astype(F32)


def node_forward(vb, agg, w_in_ref, w_out_ref):
    pre = nn(vb, w_in_ref[0:512, :]) + nn(agg, w_in_ref[512:1024, :])
    hidden = (pre * sigmoid(pre)).astype(BF16)
    normed, inv = layer_norm(nn(hidden, w_out_ref[...]))
    return pre, hidden, normed, inv


def split_store(k, scratch_ref, keep_ref, send_ref, at, rows):
    for c in range(16):
        mine = pl.multiple_of(2 * c * rows + k * rows, 16)
        other = pl.multiple_of(2 * c * rows + (1 - k) * rows, 16)
        keep_ref[c, at : at + rows, :] = scratch_ref[pl.ds(mine, rows), :]
        send_ref[c, at : at + rows, :] = scratch_ref[pl.ds(other, rows), :]


def store_gains(edge_gain, node_gain, keep_ref, send_ref):
    pad = jnp.concatenate([edge_gain, node_gain, jnp.zeros((14, 512), F32)], axis=0).astype(BF16)
    keep_ref[16, 0:16, :] = pad
    send_ref[16, 0:16, :] = pad


def node_backward(grad, vb, agg, pre, hidden, normed, inv, w_in_ref, w_out_ref, gain, g_in_ref, g_out_ref):
    grad_gain = jnp.sum(grad * normed, axis=0, keepdims=True)
    dz = layer_norm_back(grad, gain, normed, inv).astype(BF16)
    g_out_ref[...] = tn(hidden, dz).astype(BF16)
    da = (nt(dz, w_out_ref[...]) * swish_back(pre)).astype(BF16)
    g_in_ref[0:512, :] = tn(vb, da).astype(BF16)
    g_in_ref[512:1024, :] = tn(agg, da).astype(BF16)
    return grad_gain, nt(da, w_in_ref[0:512, :]), nt(da, w_in_ref[512:1024, :])


def gather_kernel(own_ref, lists_ref, vb_ref, lists, vb, o0, o1, o2, o3, sems):
    wait(Copies(sems).start((lists_ref, lists), (vb_ref.at[0], vb)))
    send_blocks(lists, own_ref[0], vb[...], (o0, o1, o2, o3))


def start_weights(copies, layer, sources, targets):
    return [copies.start((source.at[layer], target)) for source, target in zip(sources, targets)]


def first_kernel(
    own_ref, slot_ref, receiver_ref, eb_ref, vb, we_in_ref, we_out_ref, wn_in_ref, wn_out_ref, e_gain_ref, n_gain_ref,
    onehot, eb, we_in, we_out, wn_in, wn_out, e_gain, n_gain, part, proj,
    slot, receiver, sems,
):
    copies = Copies(sems)
    index = copies.start((slot_ref, slot), (receiver_ref, receiver))
    loads = start_weights(copies, 0, (we_in_ref, we_out_ref, wn_in_ref, wn_out_ref), (we_in, we_out, wn_in, wn_out))
    latent = copies.start((eb_ref.at[0], eb))
    gains = copies.start((e_gain_ref, e_gain), (n_gain_ref, n_gain))
    wait(index)
    build_onehot(onehot, slot, receiver, own_ref[0])
    wait(loads[0])
    proj[0:128, :] = nn(vb[...], we_in[1024:1536, :]).astype(BF16)
    proj[128:256, :] = nn(vb[...], we_in[512:1024, :]).astype(BF16)
    wait(latent)
    part[...] = nn(eb[...], we_in[0:512, :])
    for load in loads[1:]:
        wait(load)
    wait(gains)


def second_kernel(
    state, eb, cot_ref, we_in_ref, we_out_ref, wn_in_ref, wn_out_ref,
    cot, we_in, we_out, wn_in, wn_out, part, proj, sems,
):
    copies = Copies(sems)
    loads = start_weights(copies, 1, (we_in_ref, we_out_ref, wn_in_ref, wn_out_ref), (we_in, we_out, wn_in, wn_out))
    load = copies.start((cot_ref.at[0], cot))
    vb = state[0].astype(BF16)
    wait(loads[0])
    proj[0:128, :] = nn(vb, we_in[1024:1536, :]).astype(BF16)
    proj[128:256, :] = nn(vb, we_in[512:1024, :]).astype(BF16)
    part[...] = nn(eb[...], we_in[0:512, :])
    for handles in loads[1:]:
        wait(handles)
    wait(load)


def fill_remote(proj, near, senders, vb, blocks, w_in_ref):
    senders[0:128, :] = vb
    for n, (block, at) in enumerate(zip(blocks, (0, 0, 0, 32, 0))):
        senders[128 + 32 * n : 160 + 32 * n, :] = block[at : at + 32, :]
    proj[0:256, :] = near[...]
    proj[256:416, :] = nn(senders[128:288, :], w_in_ref[512:1024, :]).astype(BF16)
    proj[416:512, :] = jnp.zeros((96, 512), BF16)


def forward_kernel(
    own_ref, count_ref, lists, vb_ref, onehot, eb, we_in, we_out, wn_in, wn_out, e_gain, n_gain, part, near, b0, b1, b2, b3, b4,
    state, sides, eb_next, saved_out, inv_out, o0, o1, o2, o3,
    proj, message, saved, inv_s, sems,
):
    own, count = own_ref[0], count_ref[0]
    vb = vb_ref[...]
    fill_remote(proj, near, sides, vb, (b0, b1, b2, b3, b4), we_in)
    gain = e_gain[0:1, :]
    copies, saves = Copies(sems), []
    for n in range(eb.shape[0] // CHUNK):
        rows = slice(n * CHUNK, (n + 1) * CHUNK)
        pre = part[rows, :] + tn(onehot[:, rows], proj[...])
        hidden = (pre * sigmoid(pre)).astype(BF16)
        normed, inv = layer_norm(nn(hidden, we_out[...]))
        m = normed * gain * live_rows(n * CHUNK, count)
        saved[0, rows, :] = pre.astype(BF16)
        saved[1, rows, :] = normed.astype(BF16)
        inv_s[rows, :] = jnp.broadcast_to(inv, (CHUNK, 128))
        message[rows, :] = m.astype(BF16)
        eb_next[rows, :] = (eb[rows, :].astype(F32) + m).astype(BF16)
        at = pl.ds(n * CHUNK, CHUNK)
        saves += copies.start(
            (saved.at[0, at], saved_out.at[0, at]), (saved.at[1, at], saved_out.at[1, at]), (inv_s.at[at], inv_out.at[at])
        )
    agg = nn(onehot[0:128, :], message[...]).astype(BF16)
    pre, _, normed, inv = node_forward(vb, agg, wn_in, wn_out)
    v = vb.astype(F32) + normed * n_gain[0:1, :]
    state[0] = v
    state[1] = pre
    state[2] = normed
    state[3] = jnp.broadcast_to(inv, (128, 512))
    sides[288:416, :] = agg
    send_blocks(lists, own, v.astype(BF16), (o0, o1, o2, o3))
    wait(saves)


def edge_tail(onehot, senders, vb, eb, h_ref, dz_ref, da_ref, we_in, g_in, g_out, outs):
    g_out[...] = tn(h_ref[...], dz_ref[...]).astype(BF16)
    g_in[0:512, :] = tn(eb[...], da_ref[...]).astype(BF16)
    gathered = nn(onehot[0:416, :], da_ref[...]).astype(BF16)
    at_receiver = gathered[0:128, :]
    at_sender = gathered[128:416, :]
    g_in[512:1024, :] = tn(senders[...], at_sender).astype(BF16)
    g_in[1024:1536, :] = tn(vb, at_receiver).astype(BF16)
    back = nt(at_sender, we_in[512:1024, :])
    swap, pair, side, far = outs
    for n, (out, at) in enumerate(((swap, 0), (pair, 0), (side, 0), (swap, 32), (far, 0))):
        out[at : at + 32, :] = back[128 + 32 * n : 160 + 32 * n, :].astype(BF16)
    return nt(at_receiver, we_in[1024:1536, :]) + back[0:128, :]


def write_grads(k, g_in, g_out, gn_in, gn_out, edge_gain, node_gain, keep, send):
    split_store(k, g_in, keep, send, 0, 48)
    split_store(k, g_out, keep, send, 48, 16)
    split_store(k, gn_in, keep, send, 64, 32)
    split_store(k, gn_out, keep, send, 96, 16)
    store_gains(edge_gain, node_gain, keep, send)


def middle_kernel(
    own_ref, count_ref, state, onehot, eb, cot, we_in, we_out, wn_in, wn_out, e_gain, n_gain, part, near, b0, b1, b2, b3, b4,
    node_out, edge_grad_out, grad_out, keep, send, o0, o1, o2, o3,
    v, edge_grad, senders, proj, message, pre_s, normed_s, inv_s, hidden_s, dz_s, da_s, g_in, g_out, gn_in, gn_out, sems,
):
    own, count = own_ref[0], count_ref[0]
    vb = state[0].astype(BF16)
    fill_remote(proj, near, senders, vb, (b0, b1, b2, b3, b4), we_in)
    gain = e_gain[1:2, :]
    chunks = eb.shape[0] // CHUNK
    for n in range(chunks):
        rows = slice(n * CHUNK, (n + 1) * CHUNK)
        pre = part[rows, :] + tn(onehot[:, rows], proj[...])
        hidden = (pre * sigmoid(pre)).astype(BF16)
        normed, inv = layer_norm(nn(hidden, we_out[...]))
        m = normed * gain * live_rows(n * CHUNK, count)
        pre_s[rows, :] = pre
        normed_s[rows, :] = normed
        inv_s[rows, :] = jnp.broadcast_to(inv, (CHUNK, 128))
        hidden_s[rows, :] = hidden
        message[rows, :] = m.astype(BF16)
    agg = nn(onehot[0:128, :], message[...]).astype(BF16)
    n_pre, n_hidden, n_normed, n_inv = node_forward(vb, agg, wn_in, wn_out)
    n_gain_row = n_gain[1:2, :]
    v[...] = state[0] + n_normed * n_gain_row
    copies = Copies(sems)
    saves = copies.start((v, node_out.at[0]))
    grad = cot[...].astype(F32)
    grad_n_gain, grad_v, grad_agg = node_backward(
        grad, vb, agg, n_pre, n_hidden, n_normed, n_inv, wn_in, wn_out, n_gain_row, gn_in, gn_out
    )
    grad_agg = grad_agg.astype(BF16)
    grad_e_gain = jnp.zeros((1, 512), F32)
    for n in range(chunks):
        rows = slice(n * CHUNK, (n + 1) * CHUNK)
        gm = tn(onehot[0:128, rows], grad_agg) * live_rows(n * CHUNK, count)
        normed = normed_s[rows, :]
        grad_e_gain += jnp.sum(gm * normed, axis=0, keepdims=True)
        dz = layer_norm_back(gm, gain, normed, inv_s[rows, 0:1]).astype(BF16)
        dz_s[rows, :] = dz
        da = (nt(dz, we_out[...]) * swish_back(pre_s[rows, :])).astype(BF16)
        da_s[rows, :] = da
        edge_grad[rows, :] = nt(da, we_in[0:512, :]).astype(BF16)
        at = pl.ds(n * CHUNK, CHUNK)
        saves += copies.start((edge_grad.at[at], edge_grad_out.at[at]))
    grad_ends = edge_tail(onehot, senders, vb, eb, hidden_s, dz_s, da_s, we_in, g_in, g_out, (o0, o1, o2, o3))
    grad_out[...] = grad + grad_v + grad_ends
    write_grads(own & 1, g_in, g_out, gn_in, gn_out, grad_e_gain, grad_n_gain, keep, send)
    wait(saves)


def backward_kernel(
    own_ref, count_ref, lists, onehot, grad_ref, r0, r1, r2, r3, eb_ref, state_ref, sides_ref, edge_grad_ref, saved_ref, inv_ref,
    we_in_ref, we_out_ref, wn_in_ref, wn_out_ref, e_gain_ref, n_gain_ref,
    grad_out, keep, send, o0, o1, o2, o3,
    eb, state, sides, edge_grad, saved, inv_s, we_in, we_out, wn_in, wn_out, e_gain, n_gain,
    hidden_s, dz_s, da_s, g_in, g_out, gn_in, gn_out, sems,
):
    own, count = own_ref[0], count_ref[0]
    copies = Copies(sems)
    node = copies.start((state_ref.at[pl.ds(1, 3)], state), (sides_ref, sides), (n_gain_ref, n_gain))
    node += copies.start((wn_out_ref.at[0], wn_out), (wn_in_ref.at[0], wn_in))
    edge = copies.start((edge_grad_ref, edge_grad), (saved_ref, saved), (inv_ref, inv_s), (e_gain_ref, e_gain), (we_out_ref.at[0], we_out))
    last = copies.start((eb_ref.at[0], eb), (we_in_ref.at[0], we_in))
    wait(node)
    vb = sides[0:128, :]
    grad = grad_ref[...] + returned(lists, own, (r0, r1, r2, r3))
    n_pre = state[0]
    n_hidden = (n_pre * sigmoid(n_pre)).astype(BF16)
    grad_n_gain, grad_v, grad_agg = node_backward(
        grad, vb, sides[288:416, :], n_pre, n_hidden, state[1], state[2], wn_in, wn_out, n_gain[0:1, :], gn_in, gn_out
    )
    grad_agg = grad_agg.astype(BF16)
    wait(edge)
    gain = e_gain[0:1, :]
    grad_e_gain = jnp.zeros((1, 512), F32)
    for n in range(eb.shape[0] // CHUNK):
        rows = slice(n * CHUNK, (n + 1) * CHUNK)
        gm = tn(onehot[0:128, rows], grad_agg) + edge_grad[rows, :].astype(F32)
        gm = gm * live_rows(n * CHUNK, count)
        normed = saved[1, rows, :].astype(F32)
        grad_e_gain += jnp.sum(gm * normed, axis=0, keepdims=True)
        dz = layer_norm_back(gm, gain, normed, inv_s[rows, 0:1]).astype(BF16)
        dz_s[rows, :] = dz
        pre = saved[0, rows, :].astype(F32)
        s = sigmoid(pre)
        hidden_s[rows, :] = (pre * s).astype(BF16)
        da_s[rows, :] = (nt(dz, we_out[...]) * (s * (1.0 + pre * (1.0 - s)))).astype(BF16)
    wait(last)
    grad_ends = edge_tail(onehot, sides.at[0:288], vb, eb, hidden_s, dz_s, da_s, we_in, g_in, g_out, (o0, o1, o2, o3))
    grad_out[...] = grad + grad_v + grad_ends
    write_grads(own & 1, g_in, g_out, gn_in, gn_out, grad_e_gain, grad_n_gain, keep, send)


def pack_kernel(keep_ref, recv_ref, out_ref, stage, packed, sems):
    gains = keep_ref[16, 0:16, :].astype(F32) + recv_ref[16, 0:16, :].astype(F32)
    for b in range(4):
        for q in range(4):
            stage[b, 112 + q : 113 + q, :] = gains[0:1, 128 * q : 128 * q + 128]
            stage[b, 116 + q : 117 + q, :] = gains[1:2, 128 * q : 128 * q + 128]
    copies = Copies(sems)
    saves = []
    for c in range(16):
        rows = keep_ref[c].astype(F32) + recv_ref[c].astype(F32)
        for b in range(4):
            for q in range(4):
                lanes = slice(128 * q, 128 * q + 128)
                at = 28 * q
                stage[b, at : at + 12, :] = rows[12 * b : 12 * b + 12, lanes]
                stage[b, at + 12 : at + 16, :] = rows[48 + 4 * b : 52 + 4 * b, lanes]
                stage[b, at + 16 : at + 24, :] = rows[64 + 8 * b : 72 + 8 * b, lanes]
                stage[b, at + 24 : at + 28, :] = rows[96 + 4 * b : 100 + 4 * b, lanes]
            packed[4 * c + b] = stage[b].astype(BF16)
        saves += copies.start((packed.at[pl.ds(4 * c, 4)], out_ref.at[pl.ds(4 * c, 4)]))
    wait(saves)


def sum_blocks(x):
    def step(n, total):
        return total + x[n].astype(F32)

    return lax.fori_loop(0, 64, step, jnp.zeros((120, 128), F32), unroll=8)


def pick_gains(rows, device):
    picks = lax.broadcasted_iota(jnp.int32, (128, 128), 0) - 4 * (device & 31)
    select = jnp.where(picks == lax.broadcasted_iota(jnp.int32, (128, 128), 1), 1.0, 0.0).astype(F32)
    return lax.dot_general(rows, select, (((1,), (0,)), ((), ())), precision=lax.Precision.HIGHEST, preferred_element_type=F32)


def sum_kernel(device_ref, x_ref, out_ref, gains_ref, x, sems):
    wait(Copies(sems).start((x_ref, x)))
    out_ref[...] = sum_blocks(x)
    gains_ref[...] = pick_gains(out_ref[112:120, :], device_ref[0])


def node_grad_kernel(own_ref, lists, grad_ref, r0, r1, r2, r3, out_ref, total, sems):
    total[...] = grad_ref[...] + returned(lists, own_ref[0], (r0, r1, r2, r3))
    wait(Copies(sems).start((total, out_ref.at[0])))


def finish_kernel(device_ref, x0_ref, total1, gains1, g_e_in, g_e_out, g_n_in, g_n_out, g_e_gain, g_n_gain, total0):
    total0[...] = sum_blocks(x0_ref)
    device = device_ref[0]
    row = lax.broadcasted_iota(jnp.int32, (8, 128), 0) - device // 32
    for layer, total in ((0, total0), (1, total1)):
        for q in range(4):
            lanes = slice(128 * q, 128 * q + 128)
            at = 28 * q
            g_e_in[:, layer, lanes] = total[at : at + 12, :]
            g_e_out[layer, :, lanes] = total[at + 12 : at + 16, :]
            g_n_in[layer, :, lanes] = total[at + 16 : at + 24, :]
            g_n_out[layer, :, lanes] = total[at + 24 : at + 28, :]
        gains = gains1[...] if layer else pick_gains(total[112:120, :], device)
        g_e_gain[layer : layer + 1, :] = jnp.sum(jnp.where(row == 0, gains, 0.0), axis=0, keepdims=True)[:, 0:4]
        g_n_gain[layer : layer + 1, :] = jnp.sum(jnp.where(row == 4, gains, 0.0), axis=0, keepdims=True)[:, 0:4]


def body(
    node_latent,
    edge_latent,
    node_cotangent,
    edge_w_in,
    edge_w_out,
    node_w_in,
    node_w_out,
    edge_gain,
    node_gain,
    edge_slot,
    edge_receiver,
    send_list,
    edge_count,
):
    width = node_latent.shape[2]
    nodes = node_latent.shape[1]
    edges = edge_slot.shape[0]
    graph = lax.axis_size("graph")
    own = lax.axis_index("graph").astype(jnp.int32)
    own_arr = own.reshape(1)
    device = (own * lax.axis_size("batch") + lax.axis_index("batch").astype(jnp.int32)).reshape(1)
    slot = edge_slot.reshape(1, edges)
    receiver = edge_receiver.reshape(1, edges)
    sds = jax.ShapeDtypeStruct
    vmem = pl.BlockSpec(memory_space=pltpu.VMEM)
    smem = pl.BlockSpec(memory_space=pltpu.SMEM)
    free = pl.BlockSpec(memory_space=pl.ANY)
    hbm = pl.BlockSpec(memory_space=pltpu.HBM)
    kept = pl.BlockSpec(memory_space=pltpu.VMEM)

    def move(block, source):
        return lax.ppermute(block, "graph", [(source(i), i) for i in range(graph)])

    def fetch(blocks):
        swap, pair, side, far = blocks
        pair = move(pair, near)
        side, far, swap = move(side, lambda i: near(i) ^ 1), move(far, lambda i: i ^ 16), move(swap, lambda i: i ^ 1)
        return swap, pair, side, move(pair, lambda i: i ^ 1), far

    def give_back(blocks):
        swap, pair, side, far = blocks
        swap = move(swap, lambda i: i ^ 1)
        side, far = move(side, lambda i: near(i ^ 1)), move(far, lambda i: i ^ 16)
        return swap, move(jnp.concatenate([pair, swap[32:64]], axis=0), near), side, far

    def call(kernel, mib, outs, scratch, specs, args):
        at = {id(hbm): pltpu.HBM, id(kept): pltpu.VMEM}
        real = {id(hbm): free, id(kept): vmem}
        shapes = [at[id(p)](o.shape, o.dtype) if id(p) in at else o for o, p in outs]
        args = [pltpu.with_memory_space_constraint(a, at[id(p)]) if id(p) in at else a for a, p in zip(args, specs)]
        return pl.pallas_call(
            kernel,
            out_shape=shapes,
            in_specs=[real.get(id(p), p) for p in specs],
            out_specs=[real.get(id(p), p) for _, p in outs],
            scratch_shapes=scratch,
            compiler_params=pltpu.CompilerParams(vmem_limit_bytes=mib * 1024 * 1024),
        )(*args)

    def vb16(*shape):
        return pltpu.VMEM(shape, BF16)

    def vf32(*shape):
        return pltpu.VMEM(shape, F32)

    def sems(n):
        return pltpu.SemaphoreType.DMA((n,))

    def ob16(*shape):
        return (sds(shape, BF16), kept)

    def of32(*shape):
        return (sds(shape, F32), kept)

    def swap(send):
        return lax.ppermute(send, "graph", [(i, i ^ 1) for i in range(graph)])

    def spread(packed):
        groups = [[(2 * c + k) * 4 + b for c in range(16) for b in range(4)] for k in range(2)]
        return lax.all_to_all(packed, ("graph", "batch"), 0, 0, tiled=True, axis_index_groups=groups)

    index_s = [pltpu.VMEM((1, edges), jnp.int32)] * 2
    weights = (edge_w_in, edge_w_out, node_w_in, node_w_out)
    weights_s = [vb16(*w.shape[1:]) for w in weights] + [vf32(*edge_gain.shape), vf32(*node_gain.shape)]
    weights_out = [ob16(*w.shape[1:]) for w in weights]
    edge_b, edge_f = vb16(edges, width), vf32(edges, width)
    grads_s = [vb16(r, width) for r in (1536, 512, 1024, 512)]
    back_out = [(sds((r, width), BF16), vmem) for r in (64, 32, 32, 32)]
    fetch_out = [(sds((r, width), BF16), vmem) for r in (32, 64, 32, 32)]
    half = (sds((17, 112, width), BF16), vmem)

    lists, vb0, *first = call(
        gather_kernel, 2, [(sds(send_list.shape, jnp.int32), kept), ob16(nodes, width)] + fetch_out, [sems(2)],
        [smem, hbm, hbm], (own_arr, send_list, node_latent),
    )
    senders0 = fetch(first)
    onehot, eb0, we_in0, we_out0, wn_in0, wn_out0, e_gain, n_gain, part0, near0 = call(
        first_kernel,
        4,
        [ob16(512, edges), ob16(edges, width)] + weights_out + [of32(*edge_gain.shape), of32(*node_gain.shape), of32(edges, width), ob16(256, width)],
        index_s + [sems(12)],
        [smem, hbm, hbm, hbm, kept] + [hbm] * 6,
        (own_arr, slot, receiver, edge_latent, vb0, *weights, edge_gain, node_gain),
    )
    weights0 = (we_in0, we_out0, wn_in0, wn_out0, e_gain, n_gain)
    state, sides, eb1, saved, inv, *second = call(
        forward_kernel,
        10,
        [of32(4, nodes, width), ob16(416, width), ob16(edges, width), (sds((2, edges, width), BF16), hbm), (sds((edges, 128), F32), hbm)] + fetch_out,
        [vb16(512, width), edge_b, vb16(2, edges, width), vf32(edges, 128), sems(16)],
        [smem, smem] + [kept] * 12 + [vmem] * 5,
        (own_arr, edge_count, lists, vb0, onehot, eb0, *weights0, part0, near0, *senders0),
    )
    senders1 = fetch(second)
    cot, we_in1, we_out1, wn_in1, wn_out1, part1, near1 = call(
        second_kernel,
        4,
        [ob16(nodes, width)] + weights_out + [of32(edges, width), ob16(256, width)],
        [sems(8)],
        [kept, kept] + [hbm] * 5,
        (state, eb1, node_cotangent, *weights),
    )
    node_out, edge_grad, grad1, keep1, send1, *back1 = call(
        middle_kernel,
        20,
        [(sds((1, nodes, width), F32), hbm), (sds((edges, width), BF16), hbm), of32(nodes, width), half, half] + back_out,
        [vf32(nodes, width), edge_b, vb16(288, width), vb16(512, width), edge_b, edge_f, edge_f, vf32(edges, 128), edge_b, edge_b, edge_b] + grads_s + [sems(8)],
        [smem, smem] + [kept] * 12 + [vmem] * 5,
        (own_arr, edge_count, state, onehot, eb1, cot, we_in1, we_out1, wn_in1, wn_out1, e_gain, n_gain, part1, near1, *senders1),
    )
    packed_out = (sds((64, 120, 128), BF16), hbm)
    pack_s = [vf32(4, 120, 128), vb16(64, 120, 128), sems(16)]
    returned1 = give_back(back1)
    (packed1,) = call(pack_kernel, 5, [packed_out], pack_s, [vmem, vmem], (keep1, swap(send1)))
    x1 = spread(packed1)
    grad0, keep0, send0, *back0 = call(
        backward_kernel,
        22,
        [(sds((nodes, width), F32), vmem), half, half] + back_out,
        [edge_b, vf32(3, nodes, width), vb16(416, width), edge_b, vb16(2, edges, width), vf32(edges, 128)] + weights_s + [edge_b, edge_b, edge_b] + grads_s + [sems(12)],
        [smem, smem, kept, kept] + [vmem] * 5 + [hbm, free, free] + [hbm] * 9,
        (own_arr, edge_count, lists, onehot, grad1, *returned1, edge_latent, state, sides, edge_grad, saved, inv, *weights, edge_gain, node_gain),
    )
    returned0 = give_back(back0)
    (packed0,) = call(pack_kernel, 5, [packed_out], pack_s, [vmem, vmem], (keep0, swap(send0)))
    x0 = spread(packed0)
    total1, gains1 = call(
        sum_kernel, 4, [of32(120, 128), of32(8, 128)], [vb16(64, 120, 128), sems(1)], [smem, free], (device, x1)
    )
    (node_grad,) = call(
        node_grad_kernel, 2, [(sds((1, nodes, width), F32), hbm)], [vf32(nodes, width), sems(1)],
        [smem, kept, vmem] + [vmem] * 4, (own_arr, lists, grad0, *returned0),
    )
    g_e_in, *grads = call(
        finish_kernel,
        4,
        [(sds((12, 2, width), F32), vmem)] + [(sds((2, r, width), F32), vmem) for r in (4, 8, 4)] + [(sds((2, 4), F32), vmem)] * 2,
        [vf32(120, 128)],
        [smem, kept, kept, kept],
        (device, x0, total1, gains1),
    )
    return (node_out, node_grad, jnp.swapaxes(g_e_in, 0, 1), *grads)


def solution(mesh):
    in_specs = (
        P("batch", "graph", None),
        P("batch", "graph", None),
        P("batch", "graph", None),
        P(),
        P(),
        P(),
        P(),
        P(),
        P(),
        P("graph"),
        P("graph"),
        P("graph", None),
        P("graph"),
    )
    out_specs = (
        P("batch", "graph", None),
        P("batch", "graph", None),
        P(None, ("graph", "batch"), None),
        P(None, ("graph", "batch"), None),
        P(None, ("graph", "batch"), None),
        P(None, ("graph", "batch"), None),
        P(None, ("graph", "batch")),
        P(None, ("graph", "batch")),
    )
    return jax.shard_map(body, mesh=mesh, in_specs=in_specs, out_specs=out_specs, check_vma=False)
```
